128 devices in a mesh: gx: 16 (over y_hi, z, core), gy: 8 (over x, y_lo).
Axes of the slice: x: 4, y: 4 (y_hi: 2, y_lo: 2; y = y_hi * 2 + y_lo), z: 4, core: 2. Of those that a mesh axis runs over, the one named last changes fastest.
Arguments:
- mesh_state: bfloat16 [256, 256, 32, 128], P('gx', 'gy'), may hold values from -6 to 6
- part_feat: bfloat16 [524288, 128], P(('gx', 'gy')), may hold values from -6 to 6
- cell_index: int32 [524288], P(('gx', 'gy')), may hold values from 0 to 16383, as said below
- pairs: int32 [2, 3145728], P(None, ('gx', 'gy')), may hold values from 0 to 4095, as said below
- dest: int32 [524288], P(('gx', 'gy')), may hold values from 0 to 8, as said below
- mass: float32 [524288], P(('gx', 'gy')), may hold values from 0.5 to 2
- velocity: float32 [3, 524288], P(None, ('gx', 'gy')), may hold values from -30 to 30
- w_enc: bfloat16 [128, 128], replicated, may hold values from -0.5 to 0.5
- w_mesh: bfloat16 [128, 128], replicated, may hold values from -0.21875 to 0.21875
- w_pair: bfloat16 [128, 256], replicated, may hold values from -0.5 to 0.5
- w_edge: bfloat16 [128, 128], replicated, may hold values from -0.5 to 0.5
- w_node: bfloat16 [256, 128], replicated, may hold values from -0.25 to 0.25
- w_accel: bfloat16 [3, 128], replicated, may hold values from -0.5 to 0.5
Outputs:
- mesh_out: bfloat16 [256, 256, 32, 128], P('gx', 'gy')
- stay_feat: bfloat16 [524288, 128], P(('gx', 'gy'))
- stay_vel: float32 [3, 524288], P(None, ('gx', 'gy'))
- arrived_feat: bfloat16 [131072, 128], P(('gx', 'gy'))
- arrived_vel: float32 [4, 131072], P(None, ('gx', 'gy'))
The draws below stay inside these ranges and needn't reach their ends.
Inputs may be any that keep to these rules, and one draw needn't show every extreme that they name: `dest`: 0 means the particle stays; k from 1 to 8 moves it in the k-th direction of the steps. At most 128 particles of one device take any one direction, and some device receives 128 particles from each of its eight neighbours. `cell_index`: A device's particles come in 8 aligned groups of 512 rows; the particles of group g lie in cells g * 2048 to (g + 1) * 2048 - 1 of the device's block. `pairs`: A device's columns come in 8 aligned groups of 3072; both rows of a column of group g name particles of the device's group g, rows g * 512 to (g + 1) * 512 - 1.
All inputs are finite; a program needn't handle non-finite values.
Results may differ from the reference program's by a relative error of at most 0.0085.
Values may be sent and summed in bfloat16 or wider, within the bound.
No kernel may reach another device: no remote copies, remote signals or barrier semaphores. Data moves between devices by JAX's collectives and lax.ppermute only.
A program may use at most 128 MiB of HBM per device.

```python
import math
import jax
import jax.numpy as jnp
from jax import lax

F = 128
C = 128
CX = 16
CY = 32
CZ = 32
PART_DEV = 4096
NBR = 6
GRP = 512
NGRP = 8
EDGE_DEV = 24576
CELLS_DEV = 16384
NX = 256
NY = 256
PARTICLES = 524288
EDGES = 3145728
N_GX = 16
N_GY = 8
DEVICES = 128


def draw_cell_index(key, part):
    span = CELLS_DEV // NGRP
    row = jnp.arange(PARTICLES, dtype=jnp.int32) % PART_DEV
    group = row // GRP
    local = jax.random.randint(jax.random.fold_in(key, 31), (PARTICLES,), 0, span)
    return (local + group * span).astype(jnp.int32)


def draw_pairs(key, part):
    column = jnp.arange(EDGES, dtype=jnp.int32) % EDGE_DEV
    group = column // (GRP * NBR)
    local = jax.random.randint(jax.random.fold_in(key, 37), (2, EDGES), 0, GRP)
    return (local + group[None, :] * GRP).astype(jnp.int32)


def draw_dest(key, part):
    keys = jax.random.split(jax.random.fold_in(key, 11), 4)
    level = jax.random.randint(keys[0], (DEVICES,), 0, 5)
    rate = 16 * jnp.left_shift(jnp.ones((DEVICES,), jnp.int32), level.astype(jnp.int32))
    target = jax.random.randint(keys[1], (), 0, DEVICES)
    target_x = target // N_GY
    target_y = target % N_GY
    device = jnp.arange(DEVICES, dtype=jnp.int32)
    rel_x = (device // N_GY - target_x + N_GX) % N_GX
    rel_y = (device % N_GY - target_y + N_GY) % N_GY
    near_x = (rel_x <= 1) | (rel_x == N_GX - 1)
    near_y = (rel_y <= 1) | (rel_y == N_GY - 1)
    forced = near_x & near_y
    pick = jax.random.randint(keys[2], (DEVICES, PART_DEV), 0, 1024)
    way = jax.random.randint(keys[3], (DEVICES, PART_DEV), 1, 9)
    cyclic = jnp.arange(PART_DEV, dtype=jnp.int32) % 8 + 1
    chosen = jnp.where(pick < rate[:, None], way, 0)
    chosen = jnp.where(forced[:, None], cyclic[None, :], chosen)
    onehot = (chosen[:, :, None] == jnp.arange(1, 9, dtype=jnp.int32)[None, None, :]).astype(jnp.int32)
    place = jnp.sum(jnp.cumsum(onehot, axis=1) * onehot, axis=2)
    capacity = PART_DEV // 32
    chosen = jnp.where(place > capacity, 0, chosen)
    return chosen.reshape(-1).astype(jnp.int32)


def draw_velocity(key, part):
    keys = jax.random.split(jax.random.fold_in(key, 23), 2)
    device = jnp.arange(PARTICLES, dtype=jnp.int32) // PART_DEV
    ramp = 1.0 + 2.0 * device.astype(jnp.float32) / max(DEVICES - 1, 1)
    common = jax.random.uniform(keys[0], (3, 1), jnp.float32, 0.5, 1.5)
    noise = jnp.clip(jax.random.normal(keys[1], (3, PARTICLES), jnp.float32), -6.0, 6.0)
    return ((noise + common) * ramp[None, :]).astype(jnp.float32)


def steps_of(rng, extent, pieces, smallest, largest):
    loudness, own = 1.0, jax.random.fold_in(rng, 6)
    for axis_at, shards_of in pieces:
        draws = jnp.exp(jax.random.uniform(jax.random.fold_in(own, axis_at), (shards_of,), jnp.float32, smallest / len(pieces), largest / len(pieces)))
        loudness = loudness * jnp.repeat(draws, extent[axis_at] // shards_of).reshape([-1 if axis == axis_at else 1 for axis in range(len(extent))])
    return loudness


def centred(stream_key, dims, scale, reach, shards=(), kind=jnp.bfloat16):
    entries = jax.random.normal(stream_key, dims, jnp.float32) * scale
    if len(shards) > 0:
        entries = steps_of(stream_key, dims, shards, -0.22, 0.18) * entries
    return jnp.clip(entries, min=-reach, max=reach).astype(kind)


def setup_inputs(seed: int = 0) -> dict:
    key_list = jax.random.split(jax.random.key(seed), 14)
    mesh_state = centred(key_list[0], (NX, NY, CZ, C), 1.0, 6.0, ((0, 16), (1, 8)))
    part_feat = centred(key_list[1], (PARTICLES, F), 1.0, 6.0, ((0, 128),))
    cell_index = draw_cell_index(jax.random.fold_in(key_list[13], 71), 0)
    pairs = draw_pairs(jax.random.fold_in(key_list[13], 71), 0)
    dest = draw_dest(jax.random.fold_in(key_list[13], 71), 0)
    mass = jnp.clip(jnp.exp(math.log(2.0) - 1.3862944 * jax.random.uniform(key_list[5], (PARTICLES,), jnp.float32) ** steps_of(key_list[5], (PARTICLES,), ((0, 128),), -0.2, 0.2)), 0.5, 2.0)
    velocity = draw_velocity(jax.random.fold_in(key_list[13], 71), 0)
    w_enc = centred(key_list[7], (F, C), F ** -0.5, 0.5)
    w_mesh = centred(key_list[8], (C, C), (6 * C) ** -0.5, 0.21875)
    w_pair = centred(key_list[9], (F, 2 * F), F ** -0.5, 0.5)
    w_edge = centred(key_list[10], (F, F), F ** -0.5, 0.5)
    w_node = centred(key_list[11], (F + C, F), (4 * F) ** -0.5, 0.25)
    w_accel = centred(key_list[12], (3, F), F ** -0.5, 0.5)
    return {"mesh_state": mesh_state, "part_feat": part_feat, "cell_index": cell_index, "pairs": pairs, "dest": dest, "mass": mass, "velocity": velocity, "w_enc": w_enc, "w_mesh": w_mesh, "w_pair": w_pair, "w_edge": w_edge, "w_node": w_node, "w_accel": w_accel}


directions = ((-1, -1), (-1, 0), (-1, 1), (0, -1), (0, 1), (1, -1), (1, 0), (1, 1))


def encode(state_rows, feat, cell, w_enc):
    deposit = jnp.zeros((state_rows.shape[0], feat.shape[1]), jnp.float32).at[cell].add(feat.astype(jnp.float32))
    deposit = deposit.astype(jnp.bfloat16)
    return (state_rows.astype(jnp.float32) + jnp.dot(deposit, w_enc, preferred_element_type=jnp.float32)).astype(jnp.bfloat16)


def zsides(field):
    padded = jnp.pad(field, [(0, 0)] * (field.ndim - 2) + [(1, 1), (0, 0)])
    return padded[..., 2:, :] + padded[..., :-2, :]


def mesh_update(centre, sides, w_mesh):
    width = centre.shape[-1]
    summed = sides.astype(jnp.bfloat16).reshape(-1, width)
    update = jnp.dot(summed, w_mesh, preferred_element_type=jnp.float32).reshape(centre.shape)
    return (centre.astype(jnp.float32) + jax.nn.silu(update)).astype(jnp.bfloat16)


def particle_step(feat, cell, pair, mesh_rows, w_pair, w_edge, w_node):
    width = feat.shape[1]
    proj = jnp.dot(feat, w_pair, preferred_element_type=jnp.float32).astype(jnp.bfloat16)
    proj_send = proj[:, :width]
    proj_recv = proj[:, width:]
    count = pair.shape[1]
    block = min(12288, count)
    turns = count // block
    senders = pair[0].reshape(turns, block)
    receivers = pair[1].reshape(turns, block)

    def edge_block(total, index):
        pre = proj_send[index[0]].astype(jnp.float32) + proj_recv[index[1]].astype(jnp.float32)
        act = jax.nn.silu(pre).astype(jnp.bfloat16)
        message = jnp.dot(act, w_edge, preferred_element_type=jnp.float32)
        return total.at[index[1]].add(message), None

    start = jnp.zeros((feat.shape[0], width), jnp.float32)
    edge_sum, _ = lax.scan(edge_block, start, (senders, receivers))
    edge_sum = edge_sum.astype(jnp.bfloat16)
    near = mesh_rows[cell]
    update = jnp.dot(edge_sum, w_node[:width], preferred_element_type=jnp.float32)
    update = update + jnp.dot(near, w_node[width:], preferred_element_type=jnp.float32)
    return (feat.astype(jnp.float32) + jax.nn.silu(update)).astype(jnp.bfloat16)


def readout(h_new, w_accel):
    return lax.dot_general(w_accel, h_new, (((1,), (1,)), ((), ())), preferred_element_type=jnp.float32)


def pack(h_new, vel1, mass, dest, cap):
    ways = jnp.arange(1, 9, dtype=jnp.int32)
    onehot = (dest[:, None] == ways[None, :]).astype(jnp.int32)
    slot = jnp.sum((jnp.cumsum(onehot, axis=0) - 1) * onehot, axis=1).astype(jnp.int32)
    group = jnp.where(dest > 0, dest - 1, 8).astype(jnp.int32)
    feats = jnp.zeros((8, cap, h_new.shape[1]), jnp.bfloat16).at[group, slot].set(h_new, mode="drop")
    extra = jnp.concatenate([vel1, mass[None, :]], axis=0).T.astype(jnp.bfloat16)
    moving = jnp.zeros((8, cap, 4), jnp.bfloat16).at[group, slot].set(extra, mode="drop")
    return feats, jnp.transpose(moving, (0, 2, 1))


def unpack(moving, drift):
    values = moving.astype(jnp.float32)
    weight = values[..., 3:4, :]
    speed = jnp.where(weight > 0, values[..., :3, :] - drift[:, None], 0.0)
    return jnp.concatenate([speed, weight], axis=-2)


def to_blocks(whole):
    width = whole.shape[-1]
    grid = whole.reshape(N_GX, CX, N_GY, CY, CZ, width).transpose(0, 2, 1, 3, 4, 5)
    return grid.reshape(N_GX * N_GY, CX * CY * CZ, width)


def from_blocks(blocks):
    width = blocks.shape[-1]
    grid = blocks.reshape(N_GX, N_GY, CX, CY, CZ, width).transpose(0, 2, 1, 3, 4, 5)
    return grid.reshape(CX * N_GX, CY * N_GY, CZ, width)


def stencil(mesh1, w_mesh):
    planes = mesh1.shape[0]

    def one_plane(xpos):
        below = lax.dynamic_index_in_dim(mesh1, (xpos + planes - 1) % planes, 0, keepdims=False).astype(jnp.float32)
        above = lax.dynamic_index_in_dim(mesh1, (xpos + 1) % planes, 0, keepdims=False).astype(jnp.float32)
        centre_raw = lax.dynamic_index_in_dim(mesh1, xpos, 0, keepdims=False)
        centre = centre_raw.astype(jnp.float32)
        sides = below + above + jnp.roll(centre, 1, axis=0) + jnp.roll(centre, -1, axis=0) + zsides(centre)
        return mesh_update(centre_raw, sides, w_mesh)

    return lax.map(one_plane, jnp.arange(planes, dtype=jnp.int32))


def reference(mesh_state, part_feat, cell_index, pairs, dest, mass, velocity, w_enc, w_mesh, w_pair, w_edge, w_node, w_accel):
    devices = N_GX * N_GY
    width = part_feat.shape[1]
    feat_b = part_feat.reshape(devices, PART_DEV, width)
    cell_b = cell_index.reshape(devices, PART_DEV)
    pairs_b = pairs.reshape(2, devices, EDGE_DEV).transpose(1, 0, 2)
    dest_b = dest.reshape(devices, PART_DEV)
    mass_b = mass.reshape(devices, PART_DEV)
    vel_b = velocity.reshape(3, devices, PART_DEV).transpose(1, 0, 2)
    state_b = to_blocks(mesh_state)
    mesh1_b = lax.map(lambda item: encode(item[0], item[1], item[2], w_enc), (state_b, feat_b, cell_b))
    mesh2 = stencil(from_blocks(mesh1_b), w_mesh)
    mesh2_b = to_blocks(mesh2)

    def one_device(item):
        feat, cell, pair, rows, speed = item
        h_new = particle_step(feat, cell, pair, rows, w_pair, w_edge, w_node)
        return h_new, speed + readout(h_new, w_accel)

    h_b, vel1_b = lax.map(one_device, (feat_b, cell_b, pairs_b, mesh2_b, vel_b))
    momentum = jnp.sum(mass_b[:, None, :] * vel1_b, axis=(0, 2))
    drift = momentum / jnp.sum(mass)
    staying = dest_b == 0
    stay_feat = jnp.where(staying[:, :, None], h_b, jnp.zeros_like(h_b)).reshape(-1, width)
    stay_vel = jnp.where(staying[:, None, :], vel1_b - drift[None, :, None], 0.0)
    stay_vel = stay_vel.transpose(1, 0, 2).reshape(3, -1)
    cap = PART_DEV // 32
    feats_b, moving_b = lax.map(lambda item: pack(item[0], item[1], item[2], item[3], cap), (h_b, vel1_b, mass_b, dest_b))
    feats_g = feats_b.reshape(N_GX, N_GY, 8, cap, width)
    moving_g = moving_b.reshape(N_GX, N_GY, 8, 4, cap)
    got_f = []
    got_m = []
    for index, offset in enumerate(directions):
        got_f.append(jnp.roll(feats_g[:, :, index], offset, axis=(0, 1)))
        got_m.append(jnp.roll(moving_g[:, :, index], offset, axis=(0, 1)))
    arrived_feat = jnp.stack(got_f, axis=2).reshape(-1, width)
    arrived = unpack(jnp.stack(got_m, axis=2), drift)
    arrived_vel = arrived.transpose(3, 0, 1, 2, 4).reshape(4, -1)
    return mesh2, stay_feat, stay_vel, arrived_feat, arrived_vel
```

```python
import jax
import jax.numpy as jnp
from jax import lax
from jax.experimental import pallas as pl
from jax.experimental.pallas import tpu as pltpu
from jax.sharding import Mesh
from jax.sharding import PartitionSpec as P

GX_GY = ("gx_0", "gx_1", "gx_2", "gy_0", "gy_1")
GX = ("gx_0", "gx_1", "gx_2")
GY = ("gy_0", "gy_1")

DIRECTIONS = ((-1, -1), (-1, 0), (-1, 1), (0, -1), (0, 1), (1, -1), (1, 0), (1, 1))

F = 128
GRP = 512
NGRP = 8
PLANE = 1024
SPAN = 2 * PLANE
EDGES = 3072
HALF = 256
CAP = 128
SENT = 144
ECHUNK = 512

bf16 = jnp.bfloat16
f32 = jnp.float32


def dot(a, b):
    return jnp.dot(a, b, preferred_element_type=f32)


def dot_nt(a, b):
    return lax.dot_general(a, b, (((1,), (1,)), ((), ())), preferred_element_type=f32)


def silu(v):
    half = 0.5 * v
    return half + half * jnp.tanh(half)


def one_hot(rows, index):
    lanes = index.shape[1]
    return jnp.where(lax.broadcasted_iota(jnp.int32, (rows, lanes), 0) == index, 1.0, 0.0).astype(bf16)


def encode_kernel(state, feat, cell, w_enc, mesh1, y_low, y_high, x_low, x_high):
    g = pl.program_id(0)
    local = cell[0] - g * SPAN
    row = local & (PLANE - 1)
    plane = (local >> 10).astype(f32)
    upper = jnp.transpose(jnp.broadcast_to(plane, (8, GRP)))[:, 0:1]
    rows = feat[...].astype(f32)
    spread = jnp.concatenate([(rows * (1.0 - upper)).astype(bf16), (rows * upper).astype(bf16)], axis=1)
    chunk = 256
    for at in range(0, PLANE, chunk):
        hot = one_hot(chunk, row - at)
        deposit = dot(hot, spread).astype(bf16)
        for p in range(2):
            here = pl.ds(p * PLANE + at, chunk)
            mesh1[here, :] = (
                state[here, :].astype(f32) + dot(deposit[:, p * F : (p + 1) * F], w_enc[...])
            ).astype(bf16)
    for p in range(2):
        y_low[p] = mesh1[pl.ds(p * PLANE, 32), :]
        y_high[p] = mesh1[pl.ds(p * PLANE + PLANE - 32, 32), :]

    @pl.when(g == 0)
    def _():
        x_low[...] = mesh1[pl.ds(0, PLANE), :]

    @pl.when(g == NGRP - 1)
    def _():
        x_high[...] = mesh1[pl.ds(PLANE, PLANE), :]


def encode(state, feat, cell3, w_enc):
    full = lambda g: (0, 0)
    part = lambda g: (g, 0)
    return pl.pallas_call(
        encode_kernel,
        grid=(NGRP,),
        in_specs=[
            pl.BlockSpec((SPAN, F), part),
            pl.BlockSpec((GRP, F), part),
            pl.BlockSpec((1, 1, GRP), lambda g: (g, 0, 0)),
            pl.BlockSpec((F, F), full),
        ],
        out_specs=[
            pl.BlockSpec((SPAN, F), part),
            pl.BlockSpec((2, 32, F), lambda g: (g, 0, 0)),
            pl.BlockSpec((2, 32, F), lambda g: (g, 0, 0)),
            pl.BlockSpec((PLANE, F), full),
            pl.BlockSpec((PLANE, F), full),
        ],
        out_shape=[
            jax.ShapeDtypeStruct((NGRP * SPAN, F), bf16),
            jax.ShapeDtypeStruct((2 * NGRP, 32, F), bf16),
            jax.ShapeDtypeStruct((2 * NGRP, 32, F), bf16),
            jax.ShapeDtypeStruct((PLANE, F), bf16),
            jax.ShapeDtypeStruct((PLANE, F), bf16),
        ],
        compiler_params=pltpu.CompilerParams(dimension_semantics=("arbitrary",)),
        name="encode",
    )(state, feat, cell3, w_enc)


def edge_kernel(feat, pairs, dest, w_pair, w_edge, edge_sum, target, before, taken):
    g = pl.program_id(0)

    @pl.when(g == 0)
    def _():
        i = lax.broadcasted_iota(jnp.int32, (GRP, GRP), 0)
        j = lax.broadcasted_iota(jnp.int32, (GRP, GRP), 1)
        before[...] = jnp.where(i < j, 1.0, 0.0).astype(bf16)
        taken[...] = jnp.zeros((8, F), f32)

    proj = jnp.transpose(dot(feat[...], w_pair[...]).astype(bf16).astype(f32)).astype(bf16)
    send = jnp.concatenate([proj[:F, :HALF], proj[:F, HALF:]], axis=0)
    recv = jnp.concatenate([proj[F:, :HALF], proj[F:, HALF:]], axis=0)
    total = jnp.zeros((HALF, 2 * F), f32)
    for at in range(0, EDGES, ECHUNK):
        s = pairs[0:1, pl.ds(at, ECHUNK)]
        r = pairs[1:2, pl.ds(at, ECHUNK)]
        hot_s = one_hot(HALF, s & (HALF - 1))
        hot_r = one_hot(HALF, r & (HALF - 1))
        up_s = (s & HALF) > 0
        up_r = (r & HALF) > 0
        from_s = dot(send, hot_s)
        from_r = dot(recv, hot_r)
        act = silu(
            jnp.where(up_s, from_s[F:], from_s[:F]) + jnp.where(up_r, from_r[F:], from_r[:F])
        )
        spread = jnp.concatenate(
            [jnp.where(up_r, 0.0, act).astype(bf16), jnp.where(up_r, act, 0.0).astype(bf16)], axis=0
        )
        total = total + dot_nt(hot_r, spread)
    summed = jnp.concatenate([total[:, :F], total[:, F:]], axis=0)
    high = summed.astype(bf16)
    low = (summed - high.astype(f32)).astype(bf16)
    edge_sum[...] = (dot(high, w_edge[...]) + dot(low, w_edge[...])).astype(bf16)

    way = dest[0]
    ways = lax.broadcasted_iota(jnp.int32, (8, GRP), 0)
    mine = jnp.where(ways + 1 == way, 1.0, 0.0)
    earlier = dot(mine.astype(bf16), before[...]) + taken[:, 0:1]
    slot = jnp.sum(mine * (earlier + (ways * CAP).astype(f32)), axis=0, keepdims=True)
    target[0] = jnp.where(way > 0, slot, -1.0).astype(jnp.int32)
    taken[...] = taken[...] + jnp.sum(mine, axis=1, keepdims=True)


def edges(feat, pairs, dest3, w_pair, w_edge):
    full = lambda g: (0, 0)
    part = lambda g: (g, 0)
    row = lambda g: (g, 0, 0)
    return pl.pallas_call(
        edge_kernel,
        grid=(NGRP,),
        in_specs=[
            pl.BlockSpec((GRP, F), part),
            pl.BlockSpec((2, EDGES), lambda g: (0, g)),
            pl.BlockSpec((1, 1, GRP), row),
            pl.BlockSpec((F, 2 * F), full),
            pl.BlockSpec((F, F), full),
        ],
        out_specs=[pl.BlockSpec((GRP, F), part), pl.BlockSpec((1, 1, GRP), row)],
        out_shape=[
            jax.ShapeDtypeStruct((NGRP * GRP, F), bf16),
            jax.ShapeDtypeStruct((NGRP, 1, GRP), jnp.int32),
        ],
        scratch_shapes=[pltpu.VMEM((GRP, GRP), bf16), pltpu.VMEM((8, F), f32)],
        compiler_params=pltpu.CompilerParams(dimension_semantics=("arbitrary",)),
        name="edges",
    )(feat, pairs, dest3, w_pair, w_edge)


def node_kernel(
    before,
    here,
    after,
    x_low,
    x_high,
    y_low,
    y_high,
    feat,
    edge_sum,
    cell,
    dest,
    target,
    mass,
    velocity,
    w_mesh,
    w_node,
    w_accel,
    mesh_out,
    stay_feat,
    vel1_out,
    totals,
    *rest,
):
    packed = rest[:8]
    moved, sums = rest[8:]
    g = pl.program_id(0)
    first = g == 0
    final = g == NGRP - 1

    @pl.when(first)
    def _():
        moved[...] = jnp.zeros_like(moved)
        sums[...] = jnp.zeros_like(sums)

    chunk = 256
    z = lax.broadcasted_iota(jnp.int32, (chunk, F), 0) & 31
    for p in range(2):
        base = p * PLANE
        for at in range(0, PLANE, chunk):
            rows = pl.ds(at, chunk)
            mine = here[pl.ds(base + at, chunk), :].astype(f32)
            if p == 0:
                below = jnp.where(first, x_low[rows, :], before[rows, :])
                above = here[pl.ds(PLANE + at, chunk), :]
            else:
                below = here[rows, :]
                above = jnp.where(final, x_high[rows, :], after[rows, :])
            if at == 0:
                left = jnp.concatenate([y_low[p], here[pl.ds(base, chunk - 32), :]], axis=0)
            else:
                left = here[pl.ds(base + at - 32, chunk), :]
            if at + chunk == PLANE:
                right = jnp.concatenate([here[pl.ds(base + at + 32, chunk - 32), :], y_high[p]], axis=0)
            else:
                right = here[pl.ds(base + at + 32, chunk), :]
            down = jnp.where(z == 0, 0.0, pltpu.roll(mine, 1, 0))
            up = jnp.where(z == 31, 0.0, pltpu.roll(mine, chunk - 1, 0))
            sides = (
                (below.astype(f32) + above.astype(f32))
                + (left.astype(f32) + right.astype(f32))
                + (down + up)
            ).astype(bf16)
            mesh_out[pl.ds(base + at, chunk), :] = (mine + silu(dot(sides, w_mesh[...]))).astype(bf16)

    local = cell[0] - g * SPAN
    way = dest[0]
    ways = lax.broadcasted_iota(jnp.int32, (8, GRP), 0)
    row = (local & (PLANE - 1)).astype(f32)
    plane = (local >> 10).astype(f32)
    stays = jnp.where(way == 0, 1.0, 0.0)
    three = jnp.where(ways == 0, row, jnp.where(ways == 1, plane, stays))
    columns = jnp.transpose(three)
    row_at = columns[:, 0:1].astype(jnp.int32)
    upper = columns[:, 1:2]
    stay = columns[:, 2:3]
    both = jnp.concatenate([mesh_out[pl.ds(0, PLANE), :], mesh_out[pl.ds(PLANE, PLANE), :]], axis=1)
    cells = lax.broadcasted_iota(jnp.int32, (GRP, PLANE), 1)
    hot = jnp.where(cells == row_at, 1.0, 0.0).astype(bf16)
    found = dot(hot, both)
    near = jnp.where(upper > 0.5, found[:, F:], found[:, :F]).astype(bf16)
    update = dot(edge_sum[...], w_node[:F, :]) + dot(near, w_node[F:, :])
    h = (feat[...].astype(f32) + silu(update)).astype(bf16)
    stay_feat[...] = jnp.where(stay > 0.5, h.astype(f32), 0.0).astype(bf16)
    vel1 = velocity[...] + dot_nt(w_accel[...], h)
    vel1_out[...] = vel1
    weight = mass[0]
    sums[0:3, :] = sums[0:3, :] + weight * vel1
    sums[3:4, :] = sums[3:4, :] + weight

    extra = jnp.concatenate([vel1, weight, jnp.zeros((F - 4, GRP), f32)], axis=0)
    wide = jnp.concatenate([h, jnp.transpose(extra).astype(bf16)], axis=1)
    to = target[0]
    for k in range(8):
        rows = pl.ds(k * CAP, CAP)
        moved[rows, :] = moved[rows, :] + dot(one_hot(CAP, to - k * CAP), wide)

    @pl.when(final)
    def _():
        totals[...] = jnp.broadcast_to(jnp.sum(sums[...], axis=1, keepdims=True), (8, F))
        for k in range(8):
            rows = pl.ds(k * CAP, CAP)
            packed[k][0:CAP, :] = moved[rows, 0:F].astype(bf16)
            packed[k][CAP:SENT, :] = jnp.transpose(moved[rows, F:])[0 : SENT - CAP].astype(bf16)


def nodes(mesh1, halos, feat, edge_sum, cell3, dest3, target, mass3, velocity, w_mesh, w_node, w_accel):
    full = lambda g: (0, 0)
    part = lambda g: (g, 0)
    row = lambda g: (g, 0, 0)
    x_low, x_high, y_low, y_high = halos
    return pl.pallas_call(
        node_kernel,
        grid=(NGRP,),
        in_specs=[
            pl.BlockSpec((PLANE, F), lambda g: (jnp.maximum(2 * g - 1, 0), 0)),
            pl.BlockSpec((SPAN, F), part),
            pl.BlockSpec((PLANE, F), lambda g: (jnp.minimum(2 * g + 2, 2 * NGRP - 1), 0)),
            pl.BlockSpec((PLANE, F), full),
            pl.BlockSpec((PLANE, F), full),
            pl.BlockSpec((2, 32, F), row),
            pl.BlockSpec((2, 32, F), row),
            pl.BlockSpec((GRP, F), part),
            pl.BlockSpec((GRP, F), part),
            pl.BlockSpec((1, 1, GRP), row),
            pl.BlockSpec((1, 1, GRP), row),
            pl.BlockSpec((1, 1, GRP), row),
            pl.BlockSpec((1, 1, GRP), row),
            pl.BlockSpec((3, GRP), lambda g: (0, g)),
            pl.BlockSpec((F, F), full),
            pl.BlockSpec((2 * F, F), full),
            pl.BlockSpec((3, F), full),
        ],
        out_specs=[
            pl.BlockSpec((SPAN, F), part),
            pl.BlockSpec((GRP, F), part),
            pl.BlockSpec((3, GRP), lambda g: (0, g)),
            pl.BlockSpec((8, F), full),
        ]
        + [pl.BlockSpec((SENT, F), full)] * 8,
        out_shape=[
            jax.ShapeDtypeStruct((NGRP * SPAN, F), bf16),
            jax.ShapeDtypeStruct((NGRP * GRP, F), bf16),
            jax.ShapeDtypeStruct((3, NGRP * GRP), f32),
            jax.ShapeDtypeStruct((8, F), f32),
        ]
        + [jax.ShapeDtypeStruct((SENT, F), bf16)] * 8,
        scratch_shapes=[pltpu.VMEM((8 * CAP, 2 * F), f32), pltpu.VMEM((8, GRP), f32)],
        compiler_params=pltpu.CompilerParams(dimension_semantics=("arbitrary",)),
        name="nodes",
    )(
        mesh1,
        mesh1,
        mesh1,
        x_low,
        x_high,
        y_low,
        y_high,
        feat,
        edge_sum,
        cell3,
        dest3,
        target,
        mass3,
        velocity,
        w_mesh,
        w_node,
        w_accel,
    )


def finish_kernel(*refs):
    got = refs[:8]
    totals, vel1, dest, arrived_feat, arrived_vel, stay_vel = refs[8:]
    drift = totals[0:3, 0:1] / totals[3:4, 0:1]
    stay_vel[...] = jnp.where(dest[...] == 0, vel1[...] - drift, 0.0)
    for k in range(8):
        arrived_feat[pl.ds(k * CAP, CAP), :] = got[k][0:CAP, :]
        extra = got[k][CAP:SENT, :].astype(f32)
        weight = extra[3:4]
        arrived_vel[0:3, pl.ds(k * CAP, CAP)] = jnp.where(weight > 0, extra[0:3] - drift, 0.0)
        arrived_vel[3:4, pl.ds(k * CAP, CAP)] = weight


def finish(got, totals, vel1, dest2):
    return pl.pallas_call(
        finish_kernel,
        out_shape=[
            jax.ShapeDtypeStruct((8 * CAP, F), bf16),
            jax.ShapeDtypeStruct((4, 8 * CAP), f32),
            jax.ShapeDtypeStruct((3, NGRP * GRP), f32),
        ],
        name="finish",
    )(*got, totals, vel1, dest2)


def ring(block, axis, step):
    size = lax.axis_size(axis)
    return lax.ppermute(block, axis, [(i, (i + step) % size) for i in range(size)])


def offset(block, dx, dy):
    nx, ny = lax.axis_size(GX), lax.axis_size(GY)
    route = [
        (i * ny + j, ((i + dx) % nx) * ny + (j + dy) % ny) for i in range(nx) for j in range(ny)
    ]
    return lax.ppermute(block, GX_GY, route)


def shards(
    mesh_state,
    part_feat,
    cell_index,
    pairs,
    dest,
    mass,
    velocity,
    w_enc,
    w_mesh,
    w_pair,
    w_edge,
    w_node,
    w_accel,
):
    shape = mesh_state.shape
    cell3 = cell_index.reshape(NGRP, 1, GRP)
    dest3 = dest.reshape(NGRP, 1, GRP)
    mass3 = mass.reshape(NGRP, 1, GRP)
    mesh1, y_first, y_last, x_first, x_last = encode(
        mesh_state.reshape(-1, F), part_feat, cell3, w_enc
    )
    halos = (ring(x_last, GX, 1), ring(x_first, GX, -1), ring(y_last, GY, 1), ring(y_first, GY, -1))
    edge_sum, target = edges(part_feat, pairs, dest3, w_pair, w_edge)
    mesh_out, stay_feat, vel1, totals, *packed = nodes(
        mesh1, halos, part_feat, edge_sum, cell3, dest3, target, mass3, velocity, w_mesh, w_node, w_accel
    )
    got = [offset(packed[k], dx, dy) for k, (dx, dy) in enumerate(DIRECTIONS)]
    totals = lax.psum(totals, GX_GY)
    arrived_feat, arrived_vel, stay_vel = finish(got, totals, vel1, dest.reshape(1, -1))
    return (mesh_out.reshape(shape), stay_feat, stay_vel, arrived_feat, arrived_vel)


def solution(mesh):
    torus = Mesh(mesh.devices.reshape(2, 4, 2, 4, 2), ("gx_0", "gx_1", "gx_2", "gy_0", "gy_1"))
    placed = (
        P(GX, GY, None, None),
        P(GX_GY, None),
        P(GX_GY),
        P(None, GX_GY),
        P(GX_GY),
        P(GX_GY),
        P(None, GX_GY),
        P(),
        P(),
        P(),
        P(),
        P(),
        P(),
    )
    return jax.shard_map(
        shards,
        mesh=torus,
        in_specs=placed,
        out_specs=(
            P(GX, GY, None, None),
            P(GX_GY, None),
            P(None, GX_GY),
            P(GX_GY, None),
            P(None, GX_GY),
        ),
        check_vma=False,
    )
```

```python
import jax
import jax.numpy as jnp
from jax import lax
from jax.experimental import pallas as pl
from jax.experimental.pallas import tpu as pltpu
from jax.sharding import Mesh
from jax.sharding import PartitionSpec as P

GX_GY = ("gx_0", "gx_1", "gx_2", "gy_0", "gy_1")
GX = ("gx_0", "gx_1", "gx_2")
GY = ("gy_0", "gy_1")

DIRECTIONS = ((-1, -1), (-1, 0), (-1, 1), (0, -1), (0, 1), (1, -1), (1, 0), (1, 1))

F = 128
GRP = 512
NGRP = 8
PLANE = 1024
SPAN = 2 * PLANE
EDGES = 3072
HALF = 256
CAP = 128
SENT = 144
ECHUNK = 512

bf16 = jnp.bfloat16
f32 = jnp.float32


def dot(a, b):
    return jnp.dot(a, b, preferred_element_type=f32)


def dot_nt(a, b):
    return lax.dot_general(a, b, (((1,), (1,)), ((), ())), preferred_element_type=f32)


def silu(v):
    half = 0.5 * v
    return half + half * jnp.tanh(half)


def one_hot(rows, index):
    lanes = index.shape[1]
    return jnp.where(lax.broadcasted_iota(jnp.int32, (rows, lanes), 0) == index, 1.0, 0.0).astype(bf16)


def encode_kernel(state, feat, cell, w_enc, mesh1, y_low, y_high, x_low, x_high):
    g = pl.program_id(0)
    local = cell[0] - g * SPAN
    row = local & (PLANE - 1)
    plane = (local >> 10).astype(f32)
    upper = jnp.transpose(jnp.broadcast_to(plane, (8, GRP)))[:, 0:1]
    rows = feat[...].astype(f32)
    spread = jnp.concatenate([(rows * (1.0 - upper)).astype(bf16), (rows * upper).astype(bf16)], axis=1)
    chunk = 256
    for at in range(0, PLANE, chunk):
        hot = one_hot(chunk, row - at)
        deposit = dot(hot, spread).astype(bf16)
        for p in range(2):
            here = pl.ds(p * PLANE + at, chunk)
            mesh1[here, :] = (
                state[here, :].astype(f32) + dot(deposit[:, p * F : (p + 1) * F], w_enc[...])
            ).astype(bf16)
    for p in range(2):
        y_low[p] = mesh1[pl.ds(p * PLANE, 32), :]
        y_high[p] = mesh1[pl.ds(p * PLANE + PLANE - 32, 32), :]

    @pl.when(g == 0)
    def _():
        x_low[...] = mesh1[pl.ds(0, PLANE), :]

    @pl.when(g == NGRP - 1)
    def _():
        x_high[...] = mesh1[pl.ds(PLANE, PLANE), :]


def encode(state, feat, cell3, w_enc):
    full = lambda g: (0, 0)
    part = lambda g: (g, 0)
    return pl.pallas_call(
        encode_kernel,
        grid=(NGRP,),
        in_specs=[
            pl.BlockSpec((SPAN, F), part),
            pl.BlockSpec((GRP, F), part),
            pl.BlockSpec((1, 1, GRP), lambda g: (g, 0, 0)),
            pl.BlockSpec((F, F), full),
        ],
        out_specs=[
            pl.BlockSpec((SPAN, F), part),
            pl.BlockSpec((2, 32, F), lambda g: (g, 0, 0)),
            pl.BlockSpec((2, 32, F), lambda g: (g, 0, 0)),
            pl.BlockSpec((PLANE, F), full),
            pl.BlockSpec((PLANE, F), full),
        ],
        out_shape=[
            jax.ShapeDtypeStruct((NGRP * SPAN, F), bf16),
            jax.ShapeDtypeStruct((2 * NGRP, 32, F), bf16),
            jax.ShapeDtypeStruct((2 * NGRP, 32, F), bf16),
            jax.ShapeDtypeStruct((PLANE, F), bf16),
            jax.ShapeDtypeStruct((PLANE, F), bf16),
        ],
        compiler_params=pltpu.CompilerParams(dimension_semantics=("arbitrary",)),
        name="encode",
    )(state, feat, cell3, w_enc)


def edge_kernel(feat, pairs, dest, w_pair, w_edge, edge_sum, target, before, taken):
    g = pl.program_id(0)

    @pl.when(g == 0)
    def _():
        i = lax.broadcasted_iota(jnp.int32, (GRP, GRP), 0)
        j = lax.broadcasted_iota(jnp.int32, (GRP, GRP), 1)
        before[...] = jnp.where(i < j, 1.0, 0.0).astype(bf16)
        taken[...] = jnp.zeros((8, F), f32)

    proj = jnp.transpose(dot(feat[...], w_pair[...]).astype(bf16).astype(f32)).astype(bf16)
    send = jnp.concatenate([proj[:F, :HALF], proj[:F, HALF:]], axis=0)
    recv = jnp.concatenate([proj[F:, :HALF], proj[F:, HALF:]], axis=0)
    total = jnp.zeros((HALF, 2 * F), f32)
    for at in range(0, EDGES, ECHUNK):
        s = pairs[0:1, pl.ds(at, ECHUNK)]
        r = pairs[1:2, pl.ds(at, ECHUNK)]
        hot_s = one_hot(HALF, s & (HALF - 1))
        hot_r = one_hot(HALF, r & (HALF - 1))
        up_s = (s & HALF) > 0
        up_r = (r & HALF) > 0
        from_s = dot(send, hot_s)
        from_r = dot(recv, hot_r)
        act = silu(
            jnp.where(up_s, from_s[F:], from_s[:F]) + jnp.where(up_r, from_r[F:], from_r[:F])
        )
        spread = jnp.concatenate(
            [jnp.where(up_r, 0.0, act).astype(bf16), jnp.where(up_r, act, 0.0).astype(bf16)], axis=0
        )
        total = total + dot_nt(hot_r, spread)
    summed = jnp.concatenate([total[:, :F], total[:, F:]], axis=0)
    high = summed.astype(bf16)
    low = (summed - high.astype(f32)).astype(bf16)
    edge_sum[...] = (dot(high, w_edge[...]) + dot(low, w_edge[...])).astype(bf16)

    way = dest[0]
    ways = lax.broadcasted_iota(jnp.int32, (8, GRP), 0)
    mine = jnp.where(ways + 1 == way, 1.0, 0.0)
    earlier = dot(mine.astype(bf16), before[...]) + taken[:, 0:1]
    slot = jnp.sum(mine * (earlier + (ways * CAP).astype(f32)), axis=0, keepdims=True)
    target[0] = jnp.where(way > 0, slot, -1.0).astype(jnp.int32)
    taken[...] = taken[...] + jnp.sum(mine, axis=1, keepdims=True)


def edges(feat, pairs, dest3, w_pair, w_edge):
    full = lambda g: (0, 0)
    part = lambda g: (g, 0)
    row = lambda g: (g, 0, 0)
    return pl.pallas_call(
        edge_kernel,
        grid=(NGRP,),
        in_specs=[
            pl.BlockSpec((GRP, F), part),
            pl.BlockSpec((2, EDGES), lambda g: (0, g)),
            pl.BlockSpec((1, 1, GRP), row),
            pl.BlockSpec((F, 2 * F), full),
            pl.BlockSpec((F, F), full),
        ],
        out_specs=[pl.BlockSpec((GRP, F), part), pl.BlockSpec((1, 1, GRP), row)],
        out_shape=[
            jax.ShapeDtypeStruct((NGRP * GRP, F), bf16),
            jax.ShapeDtypeStruct((NGRP, 1, GRP), jnp.int32),
        ],
        scratch_shapes=[pltpu.VMEM((GRP, GRP), bf16), pltpu.VMEM((8, F), f32)],
        compiler_params=pltpu.CompilerParams(dimension_semantics=("arbitrary",)),
        name="edges",
    )(feat, pairs, dest3, w_pair, w_edge)


def node_kernel(
    before,
    here,
    after,
    x_low,
    x_high,
    y_low,
    y_high,
    feat,
    edge_sum,
    cell,
    dest,
    target,
    mass,
    velocity,
    w_mesh,
    w_node,
    w_accel,
    mesh_out,
    stay_feat,
    vel1_out,
    totals,
    *rest,
):
    packed = rest[:8]
    moved, sums = rest[8:]
    g = pl.program_id(0)
    first = g == 0
    final = g == NGRP - 1

    @pl.when(first)
    def _():
        moved[...] = jnp.zeros_like(moved)
        sums[...] = jnp.zeros_like(sums)

    chunk = 256
    z = lax.broadcasted_iota(jnp.int32, (chunk, F), 0) & 31
    for p in range(2):
        base = p * PLANE
        for at in range(0, PLANE, chunk):
            rows = pl.ds(at, chunk)
            mine = here[pl.ds(base + at, chunk), :].astype(f32)
            if p == 0:
                below = jnp.where(first, x_low[rows, :], before[rows, :])
                above = here[pl.ds(PLANE + at, chunk), :]
            else:
                below = here[rows, :]
                above = jnp.where(final, x_high[rows, :], after[rows, :])
            if at == 0:
                left = jnp.concatenate([y_low[p], here[pl.ds(base, chunk - 32), :]], axis=0)
            else:
                left = here[pl.ds(base + at - 32, chunk), :]
            if at + chunk == PLANE:
                right = jnp.concatenate([here[pl.ds(base + at + 32, chunk - 32), :], y_high[p]], axis=0)
            else:
                right = here[pl.ds(base + at + 32, chunk), :]
            down = jnp.where(z == 0, 0.0, pltpu.roll(mine, 1, 0))
            up = jnp.where(z == 31, 0.0, pltpu.roll(mine, chunk - 1, 0))
            sides = (
                (below.astype(f32) + above.astype(f32))
                + (left.astype(f32) + right.astype(f32))
                + (down + up)
            ).astype(bf16)
            mesh_out[pl.ds(base + at, chunk), :] = (mine + silu(dot(sides, w_mesh[...]))).astype(bf16)

    local = cell[0] - g * SPAN
    way = dest[0]
    ways = lax.broadcasted_iota(jnp.int32, (8, GRP), 0)
    row = (local & (PLANE - 1)).astype(f32)
    plane = (local >> 10).astype(f32)
    stays = jnp.where(way == 0, 1.0, 0.0)
    three = jnp.where(ways == 0, row, jnp.where(ways == 1, plane, stays))
    columns = jnp.transpose(three)
    row_at = columns[:, 0:1].astype(jnp.int32)
    upper = columns[:, 1:2]
    stay = columns[:, 2:3]
    both = jnp.concatenate([mesh_out[pl.ds(0, PLANE), :], mesh_out[pl.ds(PLANE, PLANE), :]], axis=1)
    cells = lax.broadcasted_iota(jnp.int32, (GRP, PLANE), 1)
    hot = jnp.where(cells == row_at, 1.0, 0.0).astype(bf16)
    found = dot(hot, both)
    near = jnp.where(upper > 0.5, found[:, F:], found[:, :F]).astype(bf16)
    update = dot(edge_sum[...], w_node[:F, :]) + dot(near, w_node[F:, :])
    h = (feat[...].astype(f32) + silu(update)).astype(bf16)
    stay_feat[...] = jnp.where(stay > 0.5, h.astype(f32), 0.0).astype(bf16)
    vel1 = velocity[...] + dot_nt(w_accel[...], h)
    vel1_out[...] = vel1
    weight = mass[0]
    sums[0:3, :] = sums[0:3, :] + weight * vel1
    sums[3:4, :] = sums[3:4, :] + weight

    extra = jnp.concatenate([vel1, weight, jnp.zeros((F - 4, GRP), f32)], axis=0)
    wide = jnp.concatenate([h, jnp.transpose(extra).astype(bf16)], axis=1)
    to = target[0]
    for k in range(8):
        rows = pl.ds(k * CAP, CAP)
        moved[rows, :] = moved[rows, :] + dot(one_hot(CAP, to - k * CAP), wide)

    @pl.when(final)
    def _():
        totals[...] = jnp.broadcast_to(jnp.sum(sums[...], axis=1, keepdims=True), (8, F))
        for k in range(8):
            rows = pl.ds(k * CAP, CAP)
            packed[k][0:CAP, :] = moved[rows, 0:F].astype(bf16)
            packed[k][CAP:SENT, :] = jnp.transpose(moved[rows, F:])[0 : SENT - CAP].astype(bf16)


def nodes(mesh1, halos, feat, edge_sum, cell3, dest3, target, mass3, velocity, w_mesh, w_node, w_accel):
    full = lambda g: (0, 0)
    part = lambda g: (g, 0)
    row = lambda g: (g, 0, 0)
    x_low, x_high, y_low, y_high = halos
    return pl.pallas_call(
        node_kernel,
        grid=(NGRP,),
        in_specs=[
            pl.BlockSpec((PLANE, F), lambda g: (jnp.maximum(2 * g - 1, 0), 0)),
            pl.BlockSpec((SPAN, F), part),
            pl.BlockSpec((PLANE, F), lambda g: (jnp.minimum(2 * g + 2, 2 * NGRP - 1), 0)),
            pl.BlockSpec((PLANE, F), full),
            pl.BlockSpec((PLANE, F), full),
            pl.BlockSpec((2, 32, F), row),
            pl.BlockSpec((2, 32, F), row),
            pl.BlockSpec((GRP, F), part),
            pl.BlockSpec((GRP, F), part),
            pl.BlockSpec((1, 1, GRP), row),
            pl.BlockSpec((1, 1, GRP), row),
            pl.BlockSpec((1, 1, GRP), row),
            pl.BlockSpec((1, 1, GRP), row),
            pl.BlockSpec((3, GRP), lambda g: (0, g)),
            pl.BlockSpec((F, F), full),
            pl.BlockSpec((2 * F, F), full),
            pl.BlockSpec((3, F), full),
        ],
        out_specs=[
            pl.BlockSpec((SPAN, F), part),
            pl.BlockSpec((GRP, F), part),
            pl.BlockSpec((3, GRP), lambda g: (0, g)),
            pl.BlockSpec((8, F), full),
        ]
        + [pl.BlockSpec((SENT, F), full)] * 8,
        out_shape=[
            jax.ShapeDtypeStruct((NGRP * SPAN, F), bf16),
            jax.ShapeDtypeStruct((NGRP * GRP, F), bf16),
            jax.ShapeDtypeStruct((3, NGRP * GRP), f32),
            jax.ShapeDtypeStruct((8, F), f32),
        ]
        + [jax.ShapeDtypeStruct((SENT, F), bf16)] * 8,
        scratch_shapes=[pltpu.VMEM((8 * CAP, 2 * F), f32), pltpu.VMEM((8, GRP), f32)],
        compiler_params=pltpu.CompilerParams(dimension_semantics=("arbitrary",)),
        name="nodes",
    )(
        mesh1,
        mesh1,
        mesh1,
        x_low,
        x_high,
        y_low,
        y_high,
        feat,
        edge_sum,
        cell3,
        dest3,
        target,
        mass3,
        velocity,
        w_mesh,
        w_node,
        w_accel,
    )


def finish_kernel(*refs):
    got = refs[:8]
    totals, vel1, dest, arrived_feat, arrived_vel, stay_vel = refs[8:]
    drift = totals[0:3, 0:1] / totals[3:4, 0:1]
    stay_vel[...] = jnp.where(dest[...] == 0, vel1[...] - drift, 0.0)
    for k in range(8):
        arrived_feat[pl.ds(k * CAP, CAP), :] = got[k][0:CAP, :]
        extra = got[k][CAP:SENT, :].astype(f32)
        weight = extra[3:4]
        arrived_vel[0:3, pl.ds(k * CAP, CAP)] = jnp.where(weight > 0, extra[0:3] - drift, 0.0)
        arrived_vel[3:4, pl.ds(k * CAP, CAP)] = weight


def finish(got, totals, vel1, dest2):
    return pl.pallas_call(
        finish_kernel,
        out_shape=[
            jax.ShapeDtypeStruct((8 * CAP, F), bf16),
            jax.ShapeDtypeStruct((4, 8 * CAP), f32),
            jax.ShapeDtypeStruct((3, NGRP * GRP), f32),
        ],
        name="finish",
    )(*got, totals, vel1, dest2)


def ring(block, axis, step):
    size = lax.axis_size(axis)
    return lax.ppermute(block, axis, [(i, (i + step) % size) for i in range(size)])


def offset(block, dx, dy):
    nx, ny = lax.axis_size(GX), lax.axis_size(GY)
    route = [
        (i * ny + j, ((i + dx) % nx) * ny + (j + dy) % ny) for i in range(nx) for j in range(ny)
    ]
    return lax.ppermute(block, GX_GY, route)


def summed(totals):
    devices = lax.axis_size(GX_GY)
    copies = jnp.broadcast_to(totals[0:4, 0], (devices, 1, 4))
    everyone = lax.all_to_all(copies, GX_GY, 0, 0).reshape(devices, 4)
    return jnp.broadcast_to(jnp.sum(everyone, axis=0)[:, None], (4, F))


def shards(
    mesh_state,
    part_feat,
    cell_index,
    pairs,
    dest,
    mass,
    velocity,
    w_enc,
    w_mesh,
    w_pair,
    w_edge,
    w_node,
    w_accel,
):
    shape = mesh_state.shape
    cell3 = cell_index.reshape(NGRP, 1, GRP)
    dest3 = dest.reshape(NGRP, 1, GRP)
    mass3 = mass.reshape(NGRP, 1, GRP)
    mesh1, y_first, y_last, x_first, x_last = encode(
        mesh_state.reshape(-1, F), part_feat, cell3, w_enc
    )
    halos = (ring(x_last, GX, 1), ring(x_first, GX, -1), ring(y_last, GY, 1), ring(y_first, GY, -1))
    edge_sum, target = edges(part_feat, pairs, dest3, w_pair, w_edge)
    mesh_out, stay_feat, vel1, totals, *packed = nodes(
        mesh1, halos, part_feat, edge_sum, cell3, dest3, target, mass3, velocity, w_mesh, w_node, w_accel
    )
    got = [offset(packed[k], dx, dy) for k, (dx, dy) in enumerate(DIRECTIONS)]
    totals = summed(totals)
    arrived_feat, arrived_vel, stay_vel = finish(got, totals, vel1, dest.reshape(1, -1))
    return (mesh_out.reshape(shape), stay_feat, stay_vel, arrived_feat, arrived_vel)


def solution(mesh):
    torus = Mesh(mesh.devices.reshape(2, 4, 2, 4, 2), ("gx_0", "gx_1", "gx_2", "gy_0", "gy_1"))
    placed = (
        P(GX, GY, None, None),
        P(GX_GY, None),
        P(GX_GY),
        P(None, GX_GY),
        P(GX_GY),
        P(GX_GY),
        P(None, GX_GY),
        P(),
        P(),
        P(),
        P(),
        P(),
        P(),
    )
    return jax.shard_map(
        shards,
        mesh=torus,
        in_specs=placed,
        out_specs=(
            P(GX, GY, None, None),
            P(GX_GY, None),
            P(None, GX_GY),
            P(GX_GY, None),
            P(None, GX_GY),
        ),
        check_vma=False,
    )
```

```python
import jax
import jax.numpy as jnp
from jax import lax
from jax.experimental import pallas as pl
from jax.experimental.pallas import tpu as pltpu
from jax.sharding import Mesh
from jax.sharding import PartitionSpec as P


GX_GY = ("gx_0", "gx_1", "gx_2", "gy_0", "gy_1")
GX = ("gx_0", "gx_1", "gx_2")
GY = ("gy_0", "gy_1")

DIRECTIONS = ((-1, -1), (-1, 0), (-1, 1), (0, -1), (0, 1), (1, -1), (1, 0), (1, 1))

F = 128
GRP = 512
NGRP = 8
PLANE = 1024
SPAN = 2 * PLANE
EDGES = 3072
HALF = 256
CAP = 128
SENT = 144
ECHUNK = 1024

bf16 = jnp.bfloat16
f32 = jnp.float32


def dot(a, b):
    return jnp.dot(a, b, preferred_element_type=f32)


def dot_nt(a, b):
    return lax.dot_general(a, b, (((1,), (1,)), ((), ())), preferred_element_type=f32)


def silu(v):
    half = 0.5 * v
    return half + half * jnp.tanh(half)


def one_hot(rows, index):
    lanes = index.shape[1]
    mine = lax.broadcasted_iota(jnp.int16, (rows, lanes), 0) == index.astype(jnp.int16)
    return jnp.where(mine, jnp.ones((), bf16), jnp.zeros((), bf16))


def encode_kernel(state, feat, cell, w_enc, mesh1, y_low, y_high, x_low, x_high, w_both):
    g = pl.program_id(0)

    @pl.when(g == 0)
    def _():
        w_both[...] = jnp.zeros_like(w_both)
        w_both[0:F, 0:F] = w_enc[...]
        w_both[F:, F:] = w_enc[...]

    local = cell[0] - g * SPAN
    row = local & (PLANE - 1)
    plane = (local >> 10).astype(f32)
    upper = jnp.transpose(jnp.broadcast_to(plane, (8, GRP)))[:, 0:1]
    rows = feat[...].astype(f32)
    spread = jnp.concatenate([(rows * (1.0 - upper)).astype(bf16), (rows * upper).astype(bf16)], axis=1)
    added = dot(dot(one_hot(PLANE, row), spread).astype(bf16), w_both[...])
    for p in range(2):
        here = pl.ds(p * PLANE, PLANE)
        mesh1[here, :] = (state[here, :].astype(f32) + added[:, p * F : (p + 1) * F]).astype(bf16)
    for p in range(2):
        y_low[p] = mesh1[pl.ds(p * PLANE, 32), :]
        y_high[p] = mesh1[pl.ds(p * PLANE + PLANE - 32, 32), :]

    @pl.when(g == 0)
    def _():
        x_low[...] = mesh1[pl.ds(0, PLANE), :]

    @pl.when(g == NGRP - 1)
    def _():
        x_high[...] = mesh1[pl.ds(PLANE, PLANE), :]


def encode(state, feat, cell3, w_enc):
    full = lambda g: (0, 0)
    part = lambda g: (g, 0)
    return pl.pallas_call(
        encode_kernel,
        grid=(NGRP,),
        in_specs=[
            pl.BlockSpec((SPAN, F), part),
            pl.BlockSpec((GRP, F), part),
            pl.BlockSpec((1, 1, GRP), lambda g: (g, 0, 0)),
            pl.BlockSpec((F, F), full),
        ],
        out_specs=[
            pl.BlockSpec((SPAN, F), part),
            pl.BlockSpec((2, 32, F), lambda g: (g, 0, 0)),
            pl.BlockSpec((2, 32, F), lambda g: (g, 0, 0)),
            pl.BlockSpec((PLANE, F), full),
            pl.BlockSpec((PLANE, F), full),
        ],
        out_shape=[
            jax.ShapeDtypeStruct((NGRP * SPAN, F), bf16),
            jax.ShapeDtypeStruct((2 * NGRP, 32, F), bf16),
            jax.ShapeDtypeStruct((2 * NGRP, 32, F), bf16),
            jax.ShapeDtypeStruct((PLANE, F), bf16),
            jax.ShapeDtypeStruct((PLANE, F), bf16),
        ],
        scratch_shapes=[pltpu.VMEM((2 * F, 2 * F), bf16)],
        compiler_params=pltpu.CompilerParams(dimension_semantics=("arbitrary",)),
        name="encode",
    )(state, feat, cell3, w_enc)


def edge_kernel(feat, pairs, dest, w_pair, w_edge, edge_sum, target, before, taken):
    g = pl.program_id(0)

    @pl.when(g == 0)
    def _():
        i = lax.broadcasted_iota(jnp.int32, (GRP, GRP), 0)
        j = lax.broadcasted_iota(jnp.int32, (GRP, GRP), 1)
        before[...] = jnp.where(i < j, 1.0, 0.0).astype(bf16)
        taken[...] = jnp.zeros((8, F), f32)

    proj = jnp.transpose(dot(feat[...], w_pair[...]).astype(bf16).astype(f32)).astype(bf16)
    send = jnp.concatenate([proj[:F, :HALF], proj[:F, HALF:]], axis=0)
    recv = jnp.concatenate([proj[F:, :HALF], proj[F:, HALF:]], axis=0)
    total = jnp.zeros((HALF, 2 * F), f32)
    for at in range(0, EDGES, ECHUNK):
        s = pairs[0:1, pl.ds(at, ECHUNK)]
        r = pairs[1:2, pl.ds(at, ECHUNK)]
        hot_s = one_hot(HALF, s & (HALF - 1))
        hot_r = one_hot(HALF, r & (HALF - 1))
        up_s = (s & HALF) > 0
        up_r = (r & HALF) > 0
        zero = jnp.zeros((), bf16)
        from_s = dot(send, hot_s)
        from_r = dot(recv, hot_r)
        act = silu(
            jnp.where(up_s, from_s[F:], from_s[:F]) + jnp.where(up_r, from_r[F:], from_r[:F])
        )
        act = act.astype(bf16)
        spread = jnp.concatenate([jnp.where(up_r, zero, act), jnp.where(up_r, act, zero)], axis=0)
        total = total + dot(hot_r, jnp.transpose(spread))
    summed = jnp.concatenate([total[:, :F], total[:, F:]], axis=0)
    high = summed.astype(bf16)
    low = (summed - high.astype(f32)).astype(bf16)
    edge_sum[...] = (dot(high, w_edge[...]) + dot(low, w_edge[...])).astype(bf16)

    way = dest[0]
    ways = lax.broadcasted_iota(jnp.int32, (8, GRP), 0)
    mine = jnp.where(ways + 1 == way, 1.0, 0.0)
    earlier = dot(mine.astype(bf16), before[...]) + taken[:, 0:1]
    slot = jnp.sum(mine * (earlier + (ways * CAP).astype(f32)), axis=0, keepdims=True)
    target[0] = jnp.where(way > 0, slot, -1.0).astype(jnp.int32)
    taken[...] = taken[...] + jnp.sum(mine, axis=1, keepdims=True)


def edges(feat, pairs, dest3, w_pair, w_edge):
    full = lambda g: (0, 0)
    part = lambda g: (g, 0)
    row = lambda g: (g, 0, 0)
    return pl.pallas_call(
        edge_kernel,
        grid=(NGRP,),
        in_specs=[
            pl.BlockSpec((GRP, F), part),
            pl.BlockSpec((2, EDGES), lambda g: (0, g)),
            pl.BlockSpec((1, 1, GRP), row),
            pl.BlockSpec((F, 2 * F), full),
            pl.BlockSpec((F, F), full),
        ],
        out_specs=[pl.BlockSpec((GRP, F), part), pl.BlockSpec((1, 1, GRP), row)],
        out_shape=[
            jax.ShapeDtypeStruct((NGRP * GRP, F), bf16),
            jax.ShapeDtypeStruct((NGRP, 1, GRP), jnp.int32),
        ],
        scratch_shapes=[pltpu.VMEM((GRP, GRP), bf16), pltpu.VMEM((8, F), f32)],
        compiler_params=pltpu.CompilerParams(dimension_semantics=("arbitrary",)),
        name="edges",
    )(feat, pairs, dest3, w_pair, w_edge)


def node_kernel(
    before,
    here,
    after,
    x_low,
    x_high,
    y_low,
    y_high,
    feat,
    edge_sum,
    cell,
    dest,
    target,
    mass,
    velocity,
    w_mesh,
    w_node,
    w_accel,
    mesh_out,
    stay_feat,
    vel1_out,
    totals,
    *rest,
):
    packed = rest[:8]
    moved, sums = rest[8:]
    g = pl.program_id(0)
    first = g == 0
    final = g == NGRP - 1

    @pl.when(first)
    def _():
        moved[...] = jnp.zeros_like(moved)
        sums[...] = jnp.zeros_like(sums)

    chunk = 256
    z = lax.broadcasted_iota(jnp.int32, (chunk, F), 0) & 31
    for p in range(2):
        base = p * PLANE
        for at in range(0, PLANE, chunk):
            rows = pl.ds(at, chunk)
            mine = here[pl.ds(base + at, chunk), :].astype(f32)
            if p == 0:
                below = jnp.where(first, x_low[rows, :], before[rows, :])
                above = here[pl.ds(PLANE + at, chunk), :]
            else:
                below = here[rows, :]
                above = jnp.where(final, x_high[rows, :], after[rows, :])
            if at == 0:
                left = jnp.concatenate([y_low[p], here[pl.ds(base, chunk - 32), :]], axis=0)
            else:
                left = here[pl.ds(base + at - 32, chunk), :]
            if at + chunk == PLANE:
                right = jnp.concatenate([here[pl.ds(base + at + 32, chunk - 32), :], y_high[p]], axis=0)
            else:
                right = here[pl.ds(base + at + 32, chunk), :]
            down = jnp.where(z == 0, 0.0, pltpu.roll(mine, 1, 0))
            up = jnp.where(z == 31, 0.0, pltpu.roll(mine, chunk - 1, 0))
            sides = (
                (below.astype(f32) + above.astype(f32))
                + (left.astype(f32) + right.astype(f32))
                + (down + up)
            ).astype(bf16)
            mesh_out[pl.ds(base + at, chunk), :] = (mine + silu(dot(sides, w_mesh[...]))).astype(bf16)

    local = cell[0] - g * SPAN
    way = dest[0]
    ways = lax.broadcasted_iota(jnp.int32, (8, GRP), 0)
    row = (local & (PLANE - 1)).astype(f32)
    plane = (local >> 10).astype(f32)
    stays = jnp.where(way == 0, 1.0, 0.0)
    three = jnp.where(ways == 0, row, jnp.where(ways == 1, plane, stays))
    columns = jnp.transpose(three)
    row_at = columns[:, 0:1].astype(jnp.int32)
    upper = columns[:, 1:2]
    stay = columns[:, 2:3]
    both = jnp.concatenate([mesh_out[pl.ds(0, PLANE), :], mesh_out[pl.ds(PLANE, PLANE), :]], axis=1)
    cells = lax.broadcasted_iota(jnp.int32, (GRP, PLANE), 1)
    hot = jnp.where(cells == row_at, 1.0, 0.0).astype(bf16)
    found = dot(hot, both)
    near = jnp.where(upper > 0.5, found[:, F:], found[:, :F]).astype(bf16)
    update = dot(edge_sum[...], w_node[:F, :]) + dot(near, w_node[F:, :])
    h = (feat[...].astype(f32) + silu(update)).astype(bf16)
    stay_feat[...] = jnp.where(stay > 0.5, h.astype(f32), 0.0).astype(bf16)
    vel1 = velocity[...] + dot_nt(w_accel[...], h)
    vel1_out[...] = vel1
    weight = mass[0]
    sums[0:3, :] = sums[0:3, :] + weight * vel1
    sums[3:4, :] = sums[3:4, :] + weight

    extra = jnp.concatenate([vel1, weight, jnp.zeros((F - 4, GRP), f32)], axis=0)
    wide = jnp.concatenate([h, jnp.transpose(extra).astype(bf16)], axis=1)
    moved[...] = moved[...] + dot(one_hot(8 * CAP, target[0]), wide)

    @pl.when(final)
    def _():
        totals[...] = jnp.broadcast_to(jnp.sum(sums[...], axis=1, keepdims=True), (8, F))
        for k in range(8):
            rows = pl.ds(k * CAP, CAP)
            packed[k][0:CAP, :] = moved[rows, 0:F].astype(bf16)
            packed[k][CAP:SENT, :] = jnp.transpose(moved[rows, F:])[0 : SENT - CAP].astype(bf16)


def nodes(mesh1, halos, feat, edge_sum, cell3, dest3, target, mass3, velocity, w_mesh, w_node, w_accel):
    full = lambda g: (0, 0)
    part = lambda g: (g, 0)
    row = lambda g: (g, 0, 0)
    x_low, x_high, y_low, y_high = halos
    return pl.pallas_call(
        node_kernel,
        grid=(NGRP,),
        in_specs=[
            pl.BlockSpec((PLANE, F), lambda g: (jnp.maximum(2 * g - 1, 0), 0)),
            pl.BlockSpec((SPAN, F), part),
            pl.BlockSpec((PLANE, F), lambda g: (jnp.minimum(2 * g + 2, 2 * NGRP - 1), 0)),
            pl.BlockSpec((PLANE, F), full),
            pl.BlockSpec((PLANE, F), full),
            pl.BlockSpec((2, 32, F), row),
            pl.BlockSpec((2, 32, F), row),
            pl.BlockSpec((GRP, F), part),
            pl.BlockSpec((GRP, F), part),
            pl.BlockSpec((1, 1, GRP), row),
            pl.BlockSpec((1, 1, GRP), row),
            pl.BlockSpec((1, 1, GRP), row),
            pl.BlockSpec((1, 1, GRP), row),
            pl.BlockSpec((3, GRP), lambda g: (0, g)),
            pl.BlockSpec((F, F), full),
            pl.BlockSpec((2 * F, F), full),
            pl.BlockSpec((3, F), full),
        ],
        out_specs=[
            pl.BlockSpec((SPAN, F), part),
            pl.BlockSpec((GRP, F), part),
            pl.BlockSpec((3, GRP), lambda g: (0, g)),
            pl.BlockSpec((8, F), full),
        ]
        + [pl.BlockSpec((SENT, F), full)] * 8,
        out_shape=[
            jax.ShapeDtypeStruct((NGRP * SPAN, F), bf16),
            jax.ShapeDtypeStruct((NGRP * GRP, F), bf16),
            jax.ShapeDtypeStruct((3, NGRP * GRP), f32),
            jax.ShapeDtypeStruct((8, F), f32),
        ]
        + [jax.ShapeDtypeStruct((SENT, F), bf16)] * 8,
        scratch_shapes=[pltpu.VMEM((8 * CAP, 2 * F), f32), pltpu.VMEM((8, GRP), f32)],
        compiler_params=pltpu.CompilerParams(dimension_semantics=("arbitrary",)),
        name="nodes",
    )(
        mesh1,
        mesh1,
        mesh1,
        x_low,
        x_high,
        y_low,
        y_high,
        feat,
        edge_sum,
        cell3,
        dest3,
        target,
        mass3,
        velocity,
        w_mesh,
        w_node,
        w_accel,
    )


def finish_kernel(*refs):
    got = refs[:8]
    totals, vel1, dest, arrived_feat, arrived_vel, stay_vel = refs[8:]
    drift = totals[0:3, 0:1] / totals[3:4, 0:1]
    stay_vel[...] = jnp.where(dest[...] == 0, vel1[...] - drift, 0.0)
    for k in range(8):
        arrived_feat[pl.ds(k * CAP, CAP), :] = got[k][0:CAP, :]
        extra = got[k][CAP:SENT, :].astype(f32)
        weight = extra[3:4]
        arrived_vel[0:3, pl.ds(k * CAP, CAP)] = jnp.where(weight > 0, extra[0:3] - drift, 0.0)
        arrived_vel[3:4, pl.ds(k * CAP, CAP)] = weight


def finish(got, totals, vel1, dest2):
    return pl.pallas_call(
        finish_kernel,
        out_shape=[
            jax.ShapeDtypeStruct((8 * CAP, F), bf16),
            jax.ShapeDtypeStruct((4, 8 * CAP), f32),
            jax.ShapeDtypeStruct((3, NGRP * GRP), f32),
        ],
        name="finish",
    )(*got, totals, vel1, dest2)


def ring(block, axis, step):
    size = lax.axis_size(axis)
    return lax.ppermute(block, axis, [(i, (i + step) % size) for i in range(size)])


def offset(block, dx, dy):
    nx, ny = lax.axis_size(GX), lax.axis_size(GY)
    route = [
        (i * ny + j, ((i + dx) % nx) * ny + (j + dy) % ny) for i in range(nx) for j in range(ny)
    ]
    return lax.ppermute(block, GX_GY, route)


def swapped(block, axis, flip):
    return lax.ppermute(block, axis, [(i, i ^ flip) for i in range(lax.axis_size(axis))])


STAGES = (("gx_2", 1), ("gy_1", 1), ("gx_1", 1), ("gy_0", 1), ("gx_1", 2), ("gy_0", 2), ("gx_0", 1))


def exchange(packed, totals):
    got = []
    for k, (dx, dy) in enumerate(DIRECTIONS):
        got.append(offset(packed[k], dx, dy))
    for axis, flip in STAGES:
        theirs = swapped(totals, axis, flip)
        totals = totals + theirs
    return got, totals


def shards(
    mesh_state,
    part_feat,
    cell_index,
    pairs,
    dest,
    mass,
    velocity,
    w_enc,
    w_mesh,
    w_pair,
    w_edge,
    w_node,
    w_accel,
):
    shape = mesh_state.shape
    cell3 = cell_index.reshape(NGRP, 1, GRP)
    dest3 = dest.reshape(NGRP, 1, GRP)
    mass3 = mass.reshape(NGRP, 1, GRP)
    mesh1, y_first, y_last, x_first, x_last = encode(
        mesh_state.reshape(-1, F), part_feat, cell3, w_enc
    )
    halos = (ring(x_last, GX, 1), ring(x_first, GX, -1), ring(y_last, GY, 1), ring(y_first, GY, -1))
    edge_sum, target = edges(part_feat, pairs, dest3, w_pair, w_edge)
    mesh_out, stay_feat, vel1, totals, *packed = nodes(
        mesh1, halos, part_feat, edge_sum, cell3, dest3, target, mass3, velocity, w_mesh, w_node, w_accel
    )
    got, totals = exchange(packed, totals)
    arrived_feat, arrived_vel, stay_vel = finish(got, totals, vel1, dest.reshape(1, -1))
    return (mesh_out.reshape(shape), stay_feat, stay_vel, arrived_feat, arrived_vel)


def solution(mesh):
    torus = Mesh(mesh.devices.reshape(2, 4, 2, 4, 2), ("gx_0", "gx_1", "gx_2", "gy_0", "gy_1"))
    placed = (
        P(GX, GY, None, None),
        P(GX_GY, None),
        P(GX_GY),
        P(None, GX_GY),
        P(GX_GY),
        P(GX_GY),
        P(None, GX_GY),
        P(),
        P(),
        P(),
        P(),
        P(),
        P(),
    )
    return jax.shard_map(
        shards,
        mesh=torus,
        in_specs=placed,
        out_specs=(
            P(GX, GY, None, None),
            P(GX_GY, None),
            P(None, GX_GY),
            P(GX_GY, None),
            P(None, GX_GY),
        ),
        check_vma=False,
    )
```

```python
import jax
import jax.numpy as jnp
from jax import lax
from jax.experimental import pallas as pl
from jax.experimental.pallas import tpu as pltpu
from jax.sharding import Mesh
from jax.sharding import PartitionSpec as P

GX_GY = ("gx_0", "gx_1", "gx_2", "gy_0", "gy_1")
GX = ("gx_0", "gx_1", "gx_2")
GY = ("gy_0", "gy_1")

PLACES = ((0, 0), (0, 1), (0, 2), (2, 0), (3, 0), (1, 0), (1, 1), (1, 2))
PARTS = (3, 3, 1, 1)

F = 128
GRP = 512
NGRP = 8
PLANE = 1024
SPAN = 2 * PLANE
EDGES = 3072
HALF = 256
CAP = 128
SENT = 144
ECHUNK = 1024

bf16 = jnp.bfloat16
f32 = jnp.float32


def dot(a, b):
    return jnp.dot(a, b, preferred_element_type=f32)


def dot_nt(a, b):
    return lax.dot_general(a, b, (((1,), (1,)), ((), ())), preferred_element_type=f32)


def silu(v):
    half = 0.5 * v
    return half + half * jnp.tanh(half)


def one_hot(rows, index):
    lanes = index.shape[1]
    mine = lax.broadcasted_iota(jnp.int16, (rows, lanes), 0) == index.astype(jnp.int16)
    return jnp.where(mine, jnp.ones((), bf16), jnp.zeros((), bf16))


def encode_kernel(state, feat, cell, w_enc, mesh1, y_low, y_high, x_low, x_high):
    g = pl.program_id(0)
    local = cell[0] - g * SPAN
    row = local & (PLANE - 1)
    plane = (local >> 10).astype(f32)
    upper = jnp.transpose(jnp.broadcast_to(plane, (8, GRP)))[:, 0:1]
    rows = dot(feat[...], w_enc[...])
    spread = jnp.concatenate([(rows * (1.0 - upper)).astype(bf16), (rows * upper).astype(bf16)], axis=1)
    added = dot(one_hot(PLANE, row), spread)
    for p in range(2):
        here = pl.ds(p * PLANE, PLANE)
        mesh1[here, :] = (state[here, :].astype(f32) + added[:, p * F : (p + 1) * F]).astype(bf16)
    for p in range(2):
        y_low[p] = mesh1[pl.ds(p * PLANE, 32), :]
        y_high[p] = mesh1[pl.ds(p * PLANE + PLANE - 32, 32), :]

    @pl.when(g == 0)
    def _():
        x_low[...] = mesh1[pl.ds(0, PLANE), :]

    @pl.when(g == NGRP - 1)
    def _():
        x_high[...] = mesh1[pl.ds(PLANE, PLANE), :]


def encode(state, feat, cell3, w_enc):
    full = lambda g: (0, 0)
    part = lambda g: (g, 0)
    return pl.pallas_call(
        encode_kernel,
        grid=(NGRP,),
        in_specs=[
            pl.BlockSpec((SPAN, F), part),
            pl.BlockSpec((GRP, F), part),
            pl.BlockSpec((1, 1, GRP), lambda g: (g, 0, 0)),
            pl.BlockSpec((F, F), full),
        ],
        out_specs=[
            pl.BlockSpec((SPAN, F), part),
            pl.BlockSpec((2, 32, F), lambda g: (g, 0, 0)),
            pl.BlockSpec((2, 32, F), lambda g: (g, 0, 0)),
            pl.BlockSpec((PLANE, F), full),
            pl.BlockSpec((PLANE, F), full),
        ],
        out_shape=[
            jax.ShapeDtypeStruct((NGRP * SPAN, F), bf16),
            jax.ShapeDtypeStruct((2 * NGRP, 32, F), bf16),
            jax.ShapeDtypeStruct((2 * NGRP, 32, F), bf16),
            jax.ShapeDtypeStruct((PLANE, F), bf16),
            jax.ShapeDtypeStruct((PLANE, F), bf16),
        ],
        compiler_params=pltpu.CompilerParams(dimension_semantics=("arbitrary",)),
        name="encode",
    )(state, feat, cell3, w_enc)


def edge_kernel(feat, pairs, dest, w_pair, w_edge, edge_sum, target, before, taken):
    g = pl.program_id(0)

    @pl.when(g == 0)
    def _():
        i = lax.broadcasted_iota(jnp.int32, (GRP, GRP), 0)
        j = lax.broadcasted_iota(jnp.int32, (GRP, GRP), 1)
        before[...] = jnp.where(i < j, 1.0, 0.0).astype(bf16)
        taken[...] = jnp.zeros((8, F), f32)

    proj = jnp.transpose(dot(feat[...], w_pair[...]).astype(bf16).astype(f32)).astype(bf16)
    send = jnp.concatenate([proj[:F, :HALF], proj[:F, HALF:]], axis=0)
    recv = jnp.concatenate([proj[F:, :HALF], proj[F:, HALF:]], axis=0)
    total = jnp.zeros((HALF, 2 * F), f32)
    for at in range(0, EDGES, ECHUNK):
        s = pairs[0:1, pl.ds(at, ECHUNK)]
        r = pairs[1:2, pl.ds(at, ECHUNK)]
        hot_s = one_hot(HALF, s & (HALF - 1))
        hot_r = one_hot(HALF, r & (HALF - 1))
        up_s = (s & HALF) > 0
        up_r = (r & HALF) > 0
        zero = jnp.zeros((), bf16)
        from_s = dot(send, hot_s)
        from_r = dot(recv, hot_r)
        act = silu(
            jnp.where(up_s, from_s[F:], from_s[:F]) + jnp.where(up_r, from_r[F:], from_r[:F])
        )
        act = act.astype(bf16)
        spread = jnp.concatenate([jnp.where(up_r, zero, act), jnp.where(up_r, act, zero)], axis=0)
        total = total + dot(hot_r, jnp.transpose(spread))
    summed = jnp.concatenate([total[:, :F], total[:, F:]], axis=0)
    high = summed.astype(bf16)
    low = (summed - high.astype(f32)).astype(bf16)
    edge_sum[...] = (dot(high, w_edge[...]) + dot(low, w_edge[...])).astype(bf16)

    way = dest[0]
    ways = lax.broadcasted_iota(jnp.int32, (8, GRP), 0)
    mine = jnp.where(ways + 1 == way, 1.0, 0.0)
    earlier = dot(mine.astype(bf16), before[...]) + taken[:, 0:1]
    slot = jnp.sum(mine * (earlier + (ways * CAP).astype(f32)), axis=0, keepdims=True)
    target[0] = jnp.where(way > 0, slot, -1.0).astype(jnp.int32)
    taken[...] = taken[...] + jnp.sum(mine, axis=1, keepdims=True)


def edges(feat, pairs, dest3, w_pair, w_edge):
    full = lambda g: (0, 0)
    part = lambda g: (g, 0)
    row = lambda g: (g, 0, 0)
    return pl.pallas_call(
        edge_kernel,
        grid=(NGRP,),
        in_specs=[
            pl.BlockSpec((GRP, F), part),
            pl.BlockSpec((2, EDGES), lambda g: (0, g)),
            pl.BlockSpec((1, 1, GRP), row),
            pl.BlockSpec((F, 2 * F), full),
            pl.BlockSpec((F, F), full),
        ],
        out_specs=[pl.BlockSpec((GRP, F), part), pl.BlockSpec((1, 1, GRP), row)],
        out_shape=[
            jax.ShapeDtypeStruct((NGRP * GRP, F), bf16),
            jax.ShapeDtypeStruct((NGRP, 1, GRP), jnp.int32),
        ],
        scratch_shapes=[pltpu.VMEM((GRP, GRP), bf16), pltpu.VMEM((8, F), f32)],
        compiler_params=pltpu.CompilerParams(dimension_semantics=("arbitrary",)),
        name="edges",
    )(feat, pairs, dest3, w_pair, w_edge)


def node_kernel(
    before,
    here,
    after,
    x_low,
    x_high,
    y_low,
    y_high,
    feat,
    edge_sum,
    cell,
    dest,
    target,
    mass,
    velocity,
    w_mesh,
    w_node,
    w_accel,
    mesh_out,
    stay_feat,
    vel1_out,
    totals,
    *rest,
):
    packed = rest[:4]
    moved, riding, sums = rest[4:]
    g = pl.program_id(0)
    first = g == 0
    final = g == NGRP - 1

    @pl.when(first)
    def _():
        moved[...] = jnp.zeros_like(moved)
        riding[...] = jnp.zeros_like(riding)
        sums[...] = jnp.zeros_like(sums)

    chunk = 256
    z = lax.broadcasted_iota(jnp.int32, (chunk, F), 0) & 31
    for p in range(2):
        base = p * PLANE
        for at in range(0, PLANE, chunk):
            rows = pl.ds(at, chunk)
            mine = here[pl.ds(base + at, chunk), :].astype(f32)
            if p == 0:
                below = jnp.where(first, x_low[rows, :], before[rows, :])
                above = here[pl.ds(PLANE + at, chunk), :]
            else:
                below = here[rows, :]
                above = jnp.where(final, x_high[rows, :], after[rows, :])
            if at == 0:
                left = jnp.concatenate([y_low[p], here[pl.ds(base, chunk - 32), :]], axis=0)
            else:
                left = here[pl.ds(base + at - 32, chunk), :]
            if at + chunk == PLANE:
                right = jnp.concatenate([here[pl.ds(base + at + 32, chunk - 32), :], y_high[p]], axis=0)
            else:
                right = here[pl.ds(base + at + 32, chunk), :]
            down = jnp.where(z == 0, 0.0, pltpu.roll(mine, 1, 0))
            up = jnp.where(z == 31, 0.0, pltpu.roll(mine, chunk - 1, 0))
            sides = (
                (below.astype(f32) + above.astype(f32))
                + (left.astype(f32) + right.astype(f32))
                + (down + up)
            ).astype(bf16)
            mesh_out[pl.ds(base + at, chunk), :] = (mine + silu(dot(sides, w_mesh[...]))).astype(bf16)

    local = cell[0] - g * SPAN
    way = dest[0]
    ways = lax.broadcasted_iota(jnp.int32, (8, GRP), 0)
    row = (local & (PLANE - 1)).astype(f32)
    plane = (local >> 10).astype(f32)
    stays = jnp.where(way == 0, 1.0, 0.0)
    three = jnp.where(ways == 0, row, jnp.where(ways == 1, plane, jnp.where(ways == 2, stays, way.astype(f32))))
    columns = jnp.transpose(three)
    row_at = columns[:, 0:1].astype(jnp.int32)
    upper = columns[:, 1:2]
    stay = columns[:, 2:3]
    both = jnp.concatenate([mesh_out[pl.ds(0, PLANE), :], mesh_out[pl.ds(PLANE, PLANE), :]], axis=1)
    cells = lax.broadcasted_iota(jnp.int32, (GRP, PLANE), 1)
    hot = jnp.where(cells == row_at, 1.0, 0.0).astype(bf16)
    found = dot(hot, both)
    near = jnp.where(upper > 0.5, found[:, F:], found[:, :F]).astype(bf16)
    update = dot(edge_sum[...], w_node[:F, :]) + dot(near, w_node[F:, :])
    h = (feat[...].astype(f32) + silu(update)).astype(bf16)
    stay_feat[...] = jnp.where(stay > 0.5, h.astype(f32), 0.0).astype(bf16)
    vel1 = velocity[...] + dot_nt(w_accel[...], h)
    vel1_out[...] = vel1
    weight = mass[0]
    sums[0:3, :] = sums[0:3, :] + weight * vel1
    sums[3:4, :] = sums[3:4, :] + weight

    extra = jnp.concatenate([vel1, weight, jnp.zeros((12, GRP), f32)], axis=0)
    extras = jnp.concatenate([jnp.where(way == k + 1, extra, 0.0) for k in range(8)], axis=0)
    extras = jnp.transpose(extras).astype(bf16)
    goes = columns[:, 3:4]
    full = h.astype(f32)
    halves = jnp.concatenate(
        [
            jnp.where((goes > 0.5) & (goes < 4.5), full, 0.0).astype(bf16),
            jnp.where(goes > 4.5, full, 0.0).astype(bf16),
        ],
        axis=1,
    )
    to = target[0]
    moved[...] = moved[...] + dot(one_hot(4 * CAP, to & (4 * CAP - 1)), halves)
    riding[...] = riding[...] + dot(one_hot(CAP, to & (CAP - 1)), extras)

    @pl.when(final)
    def _():
        column = jnp.broadcast_to(jnp.sum(sums[...], axis=1, keepdims=True), (8, F))
        totals[...] = jnp.broadcast_to(jnp.transpose(column)[0:1, 0:4], (F, 4))[:, None, :]
        rode = jnp.transpose(riding[...]).astype(bf16)
        for k in range(8):
            rows = pl.ds(k % 4 * CAP, CAP)
            lanes = pl.ds(k // 4 * F, F)
            to, place = PLACES[k]
            packed[to][pl.ds(place * SENT, CAP), :] = moved[rows, lanes].astype(bf16)
            packed[to][pl.ds(place * SENT + CAP, SENT - CAP), :] = rode[k * 16 : (k + 1) * 16]


def nodes(mesh1, halos, feat, edge_sum, cell3, dest3, target, mass3, velocity, w_mesh, w_node, w_accel):
    full = lambda g: (0, 0)
    part = lambda g: (g, 0)
    row = lambda g: (g, 0, 0)
    x_low, x_high, y_low, y_high = halos
    return pl.pallas_call(
        node_kernel,
        grid=(NGRP,),
        in_specs=[
            pl.BlockSpec((PLANE, F), lambda g: (jnp.maximum(2 * g - 1, 0), 0)),
            pl.BlockSpec((SPAN, F), part),
            pl.BlockSpec((PLANE, F), lambda g: (jnp.minimum(2 * g + 2, 2 * NGRP - 1), 0)),
            pl.BlockSpec((PLANE, F), full),
            pl.BlockSpec((PLANE, F), full),
            pl.BlockSpec((2, 32, F), row),
            pl.BlockSpec((2, 32, F), row),
            pl.BlockSpec((GRP, F), part),
            pl.BlockSpec((GRP, F), part),
            pl.BlockSpec((1, 1, GRP), row),
            pl.BlockSpec((1, 1, GRP), row),
            pl.BlockSpec((1, 1, GRP), row),
            pl.BlockSpec((1, 1, GRP), row),
            pl.BlockSpec((3, GRP), lambda g: (0, g)),
            pl.BlockSpec((F, F), full),
            pl.BlockSpec((2 * F, F), full),
            pl.BlockSpec((3, F), full),
        ],
        out_specs=[
            pl.BlockSpec((SPAN, F), part),
            pl.BlockSpec((GRP, F), part),
            pl.BlockSpec((3, GRP), lambda g: (0, g)),
            pl.BlockSpec((F, 1, 4), lambda g: (0, 0, 0)),
        ]
        + [pl.BlockSpec((n * SENT, F), full) for n in PARTS],
        out_shape=[
            jax.ShapeDtypeStruct((NGRP * SPAN, F), bf16),
            jax.ShapeDtypeStruct((NGRP * GRP, F), bf16),
            jax.ShapeDtypeStruct((3, NGRP * GRP), f32),
            jax.ShapeDtypeStruct((F, 1, 4), f32),
        ]
        + [jax.ShapeDtypeStruct((n * SENT, F), bf16) for n in PARTS],
        scratch_shapes=[pltpu.VMEM((4 * CAP, 2 * F), f32), pltpu.VMEM((CAP, F), f32), pltpu.VMEM((8, GRP), f32)],
        compiler_params=pltpu.CompilerParams(dimension_semantics=("arbitrary",)),
        name="nodes",
    )(
        mesh1,
        mesh1,
        mesh1,
        x_low,
        x_high,
        y_low,
        y_high,
        feat,
        edge_sum,
        cell3,
        dest3,
        target,
        mass3,
        velocity,
        w_mesh,
        w_node,
        w_accel,
    )


def relay_kernel(from_high, from_low, own_down, own_up, down, up):
    for ref, own, at in ((down, own_down, 0), (up, own_up, 2)):
        there = pl.ds(at * SENT, SENT)
        ref[0:SENT, :] = from_high[there, :]
        ref[SENT : 2 * SENT, :] = own[...]
        ref[2 * SENT : 3 * SENT, :] = from_low[there, :]


def relay(from_high, from_low, own_down, own_up):
    return pl.pallas_call(
        relay_kernel,
        out_shape=[jax.ShapeDtypeStruct((3 * SENT, F), bf16)] * 2,
        name="relay",
    )(from_high, from_low, own_down, own_up)


def finish_kernel(from_high, from_low, down, up, totals, vel1, dest, arrived_feat, arrived_vel, stay_vel):
    total = jnp.transpose(jnp.broadcast_to(jnp.sum(totals[...], axis=0), (8, 4)))
    drift = total[0:3, 0:1] / total[3:4, 0:1]
    stay_vel[...] = jnp.where(dest[...] == 0, vel1[...] - drift, 0.0)
    sources = (
        (down, 0),
        (from_high, 1),
        (up, 0),
        (down, 1),
        (up, 1),
        (down, 2),
        (from_low, 1),
        (up, 2),
    )
    for k, (ref, at) in enumerate(sources):
        arrived_feat[pl.ds(k * CAP, CAP), :] = ref[pl.ds(at * SENT, CAP), :]
        extra = ref[pl.ds(at * SENT + CAP, SENT - CAP), :].astype(f32)
        weight = extra[3:4]
        arrived_vel[0:3, pl.ds(k * CAP, CAP)] = jnp.where(weight > 0, extra[0:3] - drift, 0.0)
        arrived_vel[3:4, pl.ds(k * CAP, CAP)] = weight


def finish(*args):
    return pl.pallas_call(
        finish_kernel,
        out_shape=[
            jax.ShapeDtypeStruct((8 * CAP, F), bf16),
            jax.ShapeDtypeStruct((4, 8 * CAP), f32),
            jax.ShapeDtypeStruct((3, NGRP * GRP), f32),
        ],
        name="finish",
    )(*args)


def ring(block, axis, step):
    size = lax.axis_size(axis)
    return lax.ppermute(block, axis, [(i, (i + step) % size) for i in range(size)])


def shards(
    mesh_state,
    part_feat,
    cell_index,
    pairs,
    dest,
    mass,
    velocity,
    w_enc,
    w_mesh,
    w_pair,
    w_edge,
    w_node,
    w_accel,
):
    shape = mesh_state.shape
    cell3 = cell_index.reshape(NGRP, 1, GRP)
    dest3 = dest.reshape(NGRP, 1, GRP)
    mass3 = mass.reshape(NGRP, 1, GRP)
    mesh1, y_first, y_last, x_first, x_last = encode(
        mesh_state.reshape(-1, F), part_feat, cell3, w_enc
    )
    halos = (ring(x_last, GX, 1), ring(x_first, GX, -1), ring(y_last, GY, 1), ring(y_first, GY, -1))
    edge_sum, target = edges(part_feat, pairs, dest3, w_pair, w_edge)
    mesh_out, stay_feat, vel1, totals, *packed = nodes(
        mesh1, halos, part_feat, edge_sum, cell3, dest3, target, mass3, velocity, w_mesh, w_node, w_accel
    )
    to_low, to_high, own_down, own_up = packed
    from_high, from_low = ring(to_low, GX, -1), ring(to_high, GX, 1)
    totals = lax.all_to_all(totals, GX_GY, 0, 0)
    own_down, own_up, totals = lax.optimization_barrier((own_down, own_up, totals))
    down, up = relay(from_high, from_low, own_down, own_up)
    down, up = ring(down, GY, -1), ring(up, GY, 1)
    arrived_feat, arrived_vel, stay_vel = finish(
        from_high, from_low, down, up, totals, vel1, dest.reshape(1, -1)
    )
    return (mesh_out.reshape(shape), stay_feat, stay_vel, arrived_feat, arrived_vel)


def solution(mesh):
    torus = Mesh(mesh.devices.reshape(2, 4, 2, 4, 2), ("gx_0", "gx_1", "gx_2", "gy_0", "gy_1"))
    placed = (
        P(GX, GY, None, None),
        P(GX_GY, None),
        P(GX_GY),
        P(None, GX_GY),
        P(GX_GY),
        P(GX_GY),
        P(None, GX_GY),
        P(),
        P(),
        P(),
        P(),
        P(),
        P(),
    )
    return jax.shard_map(
        shards,
        mesh=torus,
        in_specs=placed,
        out_specs=(
            P(GX, GY, None, None),
            P(GX_GY, None),
            P(None, GX_GY),
            P(GX_GY, None),
            P(None, GX_GY),
        ),
        check_vma=False,
    )
```

```python
import jax
import jax.numpy as jnp
from jax import lax
from jax.experimental import pallas as pl
from jax.experimental.pallas import tpu as pltpu
from jax.sharding import Mesh
from jax.sharding import PartitionSpec as P

GX_GY = ("gx_0", "gx_1", "gx_2", "gy_0", "gy_1")
GX = ("gx_0", "gx_1", "gx_2")
GY = ("gy_0", "gy_1")

PLACES = ((0, 0), (0, 1), (0, 2), (2, 0), (3, 0), (1, 0), (1, 1), (1, 2))
PARTS = (3, 3, 1, 1)

F = 128
GRP = 512
NGRP = 8
PLANE = 1024
SPAN = 2 * PLANE
EDGES = 3072
HALF = 256
CAP = 128
SENT = 144
ECHUNK = 1024

bf16 = jnp.bfloat16
f32 = jnp.float32


def dot(a, b):
    return jnp.dot(a, b, preferred_element_type=f32)


def dot_nt(a, b):
    return lax.dot_general(a, b, (((1,), (1,)), ((), ())), preferred_element_type=f32)


def silu(v):
    half = 0.5 * v
    return half + half * jnp.tanh(half)


def one_hot(rows, index):
    lanes = index.shape[1]
    mine = lax.broadcasted_iota(jnp.int16, (rows, lanes), 0) == index.astype(jnp.int16)
    return jnp.where(mine, jnp.ones((), bf16), jnp.zeros((), bf16))


def encode_kernel(state, feat, cell, w_enc, mesh1, y_low, y_high, x_low, x_high):
    g = pl.program_id(0)
    local = cell[0] - g * SPAN
    row = local & (PLANE - 1)
    plane = (local >> 10).astype(f32)
    upper = jnp.transpose(jnp.broadcast_to(plane, (8, GRP)))[:, 0:1]
    rows = dot(feat[...], w_enc[...])
    spread = jnp.concatenate([(rows * (1.0 - upper)).astype(bf16), (rows * upper).astype(bf16)], axis=1)
    added = dot(one_hot(PLANE, row), spread)
    for p in range(2):
        here = pl.ds(p * PLANE, PLANE)
        mesh1[here, :] = (state[here, :].astype(f32) + added[:, p * F : (p + 1) * F]).astype(bf16)
    for p in range(2):
        y_low[p] = mesh1[pl.ds(p * PLANE, 32), :]
        y_high[p] = mesh1[pl.ds(p * PLANE + PLANE - 32, 32), :]

    @pl.when(g == 0)
    def _():
        x_low[...] = mesh1[pl.ds(0, PLANE), :]

    @pl.when(g == NGRP - 1)
    def _():
        x_high[...] = mesh1[pl.ds(PLANE, PLANE), :]


def encode(state, feat, cell3, w_enc):
    full = lambda g: (0, 0)
    part = lambda g: (g, 0)
    return pl.pallas_call(
        encode_kernel,
        grid=(NGRP,),
        in_specs=[
            pl.BlockSpec((SPAN, F), part),
            pl.BlockSpec((GRP, F), part),
            pl.BlockSpec((1, 1, GRP), lambda g: (g, 0, 0)),
            pl.BlockSpec((F, F), full),
        ],
        out_specs=[
            pl.BlockSpec((SPAN, F), part),
            pl.BlockSpec((2, 32, F), lambda g: (g, 0, 0)),
            pl.BlockSpec((2, 32, F), lambda g: (g, 0, 0)),
            pl.BlockSpec((PLANE, F), full),
            pl.BlockSpec((PLANE, F), full),
        ],
        out_shape=[
            jax.ShapeDtypeStruct((NGRP * SPAN, F), bf16),
            jax.ShapeDtypeStruct((2 * NGRP, 32, F), bf16),
            jax.ShapeDtypeStruct((2 * NGRP, 32, F), bf16),
            jax.ShapeDtypeStruct((PLANE, F), bf16),
            jax.ShapeDtypeStruct((PLANE, F), bf16),
        ],
        compiler_params=pltpu.CompilerParams(dimension_semantics=("arbitrary",)),
        name="encode",
    )(state, feat, cell3, w_enc)


def edge_kernel(feat, pairs, dest, w_pair, w_edge, edge_sum, target, before, taken):
    g = pl.program_id(0)

    @pl.when(g == 0)
    def _():
        i = lax.broadcasted_iota(jnp.int32, (GRP, GRP), 0)
        j = lax.broadcasted_iota(jnp.int32, (GRP, GRP), 1)
        before[...] = jnp.where(i < j, 1.0, 0.0).astype(bf16)
        taken[...] = jnp.zeros((8, F), f32)

    proj = jnp.transpose(dot(feat[...], w_pair[...]).astype(bf16).astype(f32)).astype(bf16)
    send = jnp.concatenate([proj[:F, :HALF], proj[:F, HALF:]], axis=0)
    recv = jnp.concatenate([proj[F:, :HALF], proj[F:, HALF:]], axis=0)
    total = jnp.zeros((HALF, 2 * F), f32)
    for at in range(0, EDGES, ECHUNK):
        s = pairs[0:1, pl.ds(at, ECHUNK)]
        r = pairs[1:2, pl.ds(at, ECHUNK)]
        hot_s = one_hot(HALF, s & (HALF - 1))
        hot_r = one_hot(HALF, r & (HALF - 1))
        up_s = (s & HALF) > 0
        up_r = (r & HALF) > 0
        zero = jnp.zeros((), bf16)
        from_s = dot(send, hot_s)
        from_r = dot(recv, hot_r)
        act = silu(
            jnp.where(up_s, from_s[F:], from_s[:F]) + jnp.where(up_r, from_r[F:], from_r[:F])
        )
        act = act.astype(bf16)
        spread = jnp.concatenate([jnp.where(up_r, zero, act), jnp.where(up_r, act, zero)], axis=0)
        total = total + dot(hot_r, jnp.transpose(spread))
    summed = jnp.concatenate([total[:, :F], total[:, F:]], axis=0)
    high = summed.astype(bf16)
    low = (summed - high.astype(f32)).astype(bf16)
    edge_sum[...] = (dot(high, w_edge[...]) + dot(low, w_edge[...])).astype(bf16)

    way = dest[0]
    ways = lax.broadcasted_iota(jnp.int32, (8, GRP), 0)
    mine = jnp.where(ways + 1 == way, 1.0, 0.0)
    earlier = dot(mine.astype(bf16), before[...]) + taken[:, 0:1]
    slot = jnp.sum(mine * (earlier + (ways * CAP).astype(f32)), axis=0, keepdims=True)
    target[0] = jnp.where(way > 0, slot, -1.0).astype(jnp.int32)
    taken[...] = taken[...] + jnp.sum(mine, axis=1, keepdims=True)


def edges(feat, pairs, dest3, w_pair, w_edge):
    full = lambda g: (0, 0)
    part = lambda g: (g, 0)
    row = lambda g: (g, 0, 0)
    return pl.pallas_call(
        edge_kernel,
        grid=(NGRP,),
        in_specs=[
            pl.BlockSpec((GRP, F), part),
            pl.BlockSpec((2, EDGES), lambda g: (0, g)),
            pl.BlockSpec((1, 1, GRP), row),
            pl.BlockSpec((F, 2 * F), full),
            pl.BlockSpec((F, F), full),
        ],
        out_specs=[pl.BlockSpec((GRP, F), part), pl.BlockSpec((1, 1, GRP), row)],
        out_shape=[
            jax.ShapeDtypeStruct((NGRP * GRP, F), bf16),
            jax.ShapeDtypeStruct((NGRP, 1, GRP), jnp.int32),
        ],
        scratch_shapes=[pltpu.VMEM((GRP, GRP), bf16), pltpu.VMEM((8, F), f32)],
        compiler_params=pltpu.CompilerParams(dimension_semantics=("arbitrary",)),
        name="edges",
    )(feat, pairs, dest3, w_pair, w_edge)


def node_kernel(
    before,
    here,
    after,
    x_low,
    x_high,
    y_low,
    y_high,
    feat,
    edge_sum,
    cell,
    dest,
    target,
    mass,
    velocity,
    w_mesh,
    w_node,
    w_accel,
    mesh_out,
    stay_feat,
    vel1_out,
    totals,
    *rest,
):
    packed = rest[:4]
    moved, riding, sums = rest[4:]
    g = pl.program_id(0)
    first = g == 0
    final = g == NGRP - 1

    @pl.when(first)
    def _():
        moved[...] = jnp.zeros_like(moved)
        riding[...] = jnp.zeros_like(riding)
        sums[...] = jnp.zeros_like(sums)

    chunk = 256
    z = lax.broadcasted_iota(jnp.int32, (chunk, F), 0) & 31
    for p in range(2):
        base = p * PLANE
        for at in range(0, PLANE, chunk):
            rows = pl.ds(at, chunk)
            mine = here[pl.ds(base + at, chunk), :].astype(f32)
            if p == 0:
                below = jnp.where(first, x_low[rows, :], before[rows, :])
                above = here[pl.ds(PLANE + at, chunk), :]
            else:
                below = here[rows, :]
                above = jnp.where(final, x_high[rows, :], after[rows, :])
            if at == 0:
                left = jnp.concatenate([y_low[p], here[pl.ds(base, chunk - 32), :]], axis=0)
            else:
                left = here[pl.ds(base + at - 32, chunk), :]
            if at + chunk == PLANE:
                right = jnp.concatenate([here[pl.ds(base + at + 32, chunk - 32), :], y_high[p]], axis=0)
            else:
                right = here[pl.ds(base + at + 32, chunk), :]
            down = jnp.where(z == 0, 0.0, pltpu.roll(mine, 1, 0))
            up = jnp.where(z == 31, 0.0, pltpu.roll(mine, chunk - 1, 0))
            sides = (
                (below.astype(f32) + above.astype(f32))
                + (left.astype(f32) + right.astype(f32))
                + (down + up)
            ).astype(bf16)
            mesh_out[pl.ds(base + at, chunk), :] = (mine + silu(dot(sides, w_mesh[...]))).astype(bf16)

    local = cell[0] - g * SPAN
    way = dest[0]
    ways = lax.broadcasted_iota(jnp.int32, (8, GRP), 0)
    row = (local & (PLANE - 1)).astype(f32)
    plane = (local >> 10).astype(f32)
    stays = jnp.where(way == 0, 1.0, 0.0)
    three = jnp.where(ways == 0, row, jnp.where(ways == 1, plane, jnp.where(ways == 2, stays, way.astype(f32))))
    columns = jnp.transpose(three)
    row_at = columns[:, 0:1].astype(jnp.int32)
    upper = columns[:, 1:2]
    stay = columns[:, 2:3]
    both = jnp.concatenate([mesh_out[pl.ds(0, PLANE), :], mesh_out[pl.ds(PLANE, PLANE), :]], axis=1)
    cells = lax.broadcasted_iota(jnp.int32, (GRP, PLANE), 1)
    hot = jnp.where(cells == row_at, 1.0, 0.0).astype(bf16)
    found = dot(hot, both)
    near = jnp.where(upper > 0.5, found[:, F:], found[:, :F]).astype(bf16)
    update = dot(edge_sum[...], w_node[:F, :]) + dot(near, w_node[F:, :])
    h = (feat[...].astype(f32) + silu(update)).astype(bf16)
    stay_feat[...] = jnp.where(stay > 0.5, h.astype(f32), 0.0).astype(bf16)
    vel1 = velocity[...] + dot_nt(w_accel[...], h)
    vel1_out[...] = vel1
    weight = mass[0]
    sums[0:3, :] = sums[0:3, :] + weight * vel1
    sums[3:4, :] = sums[3:4, :] + weight

    extra = jnp.concatenate([vel1, weight, jnp.zeros((12, GRP), f32)], axis=0)
    extras = jnp.concatenate([jnp.where(way == k + 1, extra, 0.0) for k in range(8)], axis=0)
    extras = jnp.transpose(extras).astype(bf16)
    goes = columns[:, 3:4]
    full = h.astype(f32)
    halves = jnp.concatenate(
        [
            jnp.where((goes > 0.5) & (goes < 4.5), full, 0.0).astype(bf16),
            jnp.where(goes > 4.5, full, 0.0).astype(bf16),
        ],
        axis=1,
    )
    to = target[0]
    moved[...] = moved[...] + dot(one_hot(4 * CAP, to & (4 * CAP - 1)), halves)
    riding[...] = riding[...] + dot(one_hot(CAP, to & (CAP - 1)), extras)

    @pl.when(final)
    def _():
        column = jnp.broadcast_to(jnp.sum(sums[...], axis=1, keepdims=True), (8, F))
        totals[...] = jnp.broadcast_to(jnp.transpose(column)[0:1, 0:4], (F, 4))[:, None, :]
        rode = jnp.transpose(riding[...]).astype(bf16)
        for k in range(8):
            rows = pl.ds(k % 4 * CAP, CAP)
            lanes = pl.ds(k // 4 * F, F)
            to, place = PLACES[k]
            packed[to][pl.ds(place * SENT, CAP), :] = moved[rows, lanes].astype(bf16)
            packed[to][pl.ds(place * SENT + CAP, SENT - CAP), :] = rode[k * 16 : (k + 1) * 16]


def nodes(mesh1, halos, feat, edge_sum, cell3, dest3, target, mass3, velocity, w_mesh, w_node, w_accel):
    full = lambda g: (0, 0)
    part = lambda g: (g, 0)
    row = lambda g: (g, 0, 0)
    x_low, x_high, y_low, y_high = halos
    return pl.pallas_call(
        node_kernel,
        grid=(NGRP,),
        in_specs=[
            pl.BlockSpec((PLANE, F), lambda g: (jnp.maximum(2 * g - 1, 0), 0)),
            pl.BlockSpec((SPAN, F), part),
            pl.BlockSpec((PLANE, F), lambda g: (jnp.minimum(2 * g + 2, 2 * NGRP - 1), 0)),
            pl.BlockSpec((PLANE, F), full),
            pl.BlockSpec((PLANE, F), full),
            pl.BlockSpec((2, 32, F), row),
            pl.BlockSpec((2, 32, F), row),
            pl.BlockSpec((GRP, F), part),
            pl.BlockSpec((GRP, F), part),
            pl.BlockSpec((1, 1, GRP), row),
            pl.BlockSpec((1, 1, GRP), row),
            pl.BlockSpec((1, 1, GRP), row),
            pl.BlockSpec((1, 1, GRP), row),
            pl.BlockSpec((3, GRP), lambda g: (0, g)),
            pl.BlockSpec((F, F), full),
            pl.BlockSpec((2 * F, F), full),
            pl.BlockSpec((3, F), full),
        ],
        out_specs=[
            pl.BlockSpec((SPAN, F), part),
            pl.BlockSpec((GRP, F), part),
            pl.BlockSpec((3, GRP), lambda g: (0, g)),
            pl.BlockSpec((F, 1, 4), lambda g: (0, 0, 0)),
        ]
        + [pl.BlockSpec((n * SENT, F), full) for n in PARTS],
        out_shape=[
            jax.ShapeDtypeStruct((NGRP * SPAN, F), bf16),
            jax.ShapeDtypeStruct((NGRP * GRP, F), bf16),
            jax.ShapeDtypeStruct((3, NGRP * GRP), f32),
            jax.ShapeDtypeStruct((F, 1, 4), f32),
        ]
        + [jax.ShapeDtypeStruct((n * SENT, F), bf16) for n in PARTS],
        scratch_shapes=[pltpu.VMEM((4 * CAP, 2 * F), f32), pltpu.VMEM((CAP, F), f32), pltpu.VMEM((8, GRP), f32)],
        compiler_params=pltpu.CompilerParams(dimension_semantics=("arbitrary",)),
        name="nodes",
    )(
        mesh1,
        mesh1,
        mesh1,
        x_low,
        x_high,
        y_low,
        y_high,
        feat,
        edge_sum,
        cell3,
        dest3,
        target,
        mass3,
        velocity,
        w_mesh,
        w_node,
        w_accel,
    )


def near(block):
    return pltpu.with_memory_space_constraint(block, pltpu.VMEM)


def relay_kernel(from_high, from_low, own_down, own_up, down, up):
    for ref, own, at in ((down, own_down, 0), (up, own_up, 2)):
        there = pl.ds(at * SENT, SENT)
        ref[0:SENT, :] = from_high[there, :]
        ref[SENT : 2 * SENT, :] = own[...]
        ref[2 * SENT : 3 * SENT, :] = from_low[there, :]


def relay(from_high, from_low, own_down, own_up):
    return pl.pallas_call(
        relay_kernel,
        out_shape=[jax.ShapeDtypeStruct((3 * SENT, F), bf16)] * 2,
        name="relay",
    )(from_high, from_low, own_down, own_up)


def finish_kernel(from_high, from_low, down, up, totals, vel1, dest, arrived_feat, arrived_vel, stay_vel):
    total = jnp.transpose(jnp.broadcast_to(jnp.sum(totals[...], axis=0), (8, 4)))
    drift = total[0:3, 0:1] / total[3:4, 0:1]
    stay_vel[...] = jnp.where(dest[...] == 0, vel1[...] - drift, 0.0)
    sources = (
        (down, 0),
        (from_high, 1),
        (up, 0),
        (down, 1),
        (up, 1),
        (down, 2),
        (from_low, 1),
        (up, 2),
    )
    for k, (ref, at) in enumerate(sources):
        arrived_feat[pl.ds(k * CAP, CAP), :] = ref[pl.ds(at * SENT, CAP), :]
        extra = ref[pl.ds(at * SENT + CAP, SENT - CAP), :].astype(f32)
        weight = extra[3:4]
        arrived_vel[0:3, pl.ds(k * CAP, CAP)] = jnp.where(weight > 0, extra[0:3] - drift, 0.0)
        arrived_vel[3:4, pl.ds(k * CAP, CAP)] = weight


def finish(*args):
    return pl.pallas_call(
        finish_kernel,
        out_shape=[
            jax.ShapeDtypeStruct((8 * CAP, F), bf16),
            jax.ShapeDtypeStruct((4, 8 * CAP), f32),
            jax.ShapeDtypeStruct((3, NGRP * GRP), f32),
        ],
        name="finish",
    )(*args)


def ring(block, axis, step):
    size = lax.axis_size(axis)
    return lax.ppermute(block, axis, [(i, (i + step) % size) for i in range(size)])


def shards(
    mesh_state,
    part_feat,
    cell_index,
    pairs,
    dest,
    mass,
    velocity,
    w_enc,
    w_mesh,
    w_pair,
    w_edge,
    w_node,
    w_accel,
):
    shape = mesh_state.shape
    cell3 = cell_index.reshape(NGRP, 1, GRP)
    dest3 = dest.reshape(NGRP, 1, GRP)
    mass3 = mass.reshape(NGRP, 1, GRP)
    mesh1, y_first, y_last, x_first, x_last = encode(
        mesh_state.reshape(-1, F), part_feat, cell3, w_enc
    )
    halos = (ring(x_last, GX, 1), ring(x_first, GX, -1), ring(y_last, GY, 1), ring(y_first, GY, -1))
    halos = tuple(near(block) for block in halos)
    edge_sum, target = edges(part_feat, pairs, dest3, w_pair, w_edge)
    mesh_out, stay_feat, vel1, totals, *packed = nodes(
        mesh1, halos, part_feat, edge_sum, cell3, dest3, target, mass3, velocity, w_mesh, w_node, w_accel
    )
    to_low, to_high, own_down, own_up = packed
    from_high, from_low = ring(to_low, GX, -1), ring(to_high, GX, 1)
    from_high, from_low = near(from_high), near(from_low)
    down, up = relay(from_high, from_low, own_down, own_up)
    down, up, totals = lax.optimization_barrier((down, up, totals))
    down, up = ring(down, GY, -1), ring(up, GY, 1)
    totals = lax.all_to_all(totals, GX_GY, 0, 0)
    down, up = near(down), near(up)
    arrived_feat, arrived_vel, stay_vel = finish(
        from_high, from_low, down, up, totals, vel1, dest.reshape(1, -1)
    )
    return (mesh_out.reshape(shape), stay_feat, stay_vel, arrived_feat, arrived_vel)


def solution(mesh):
    torus = Mesh(mesh.devices.reshape(2, 4, 2, 4, 2), ("gx_0", "gx_1", "gx_2", "gy_0", "gy_1"))
    placed = (
        P(GX, GY, None, None),
        P(GX_GY, None),
        P(GX_GY),
        P(None, GX_GY),
        P(GX_GY),
        P(GX_GY),
        P(None, GX_GY),
        P(),
        P(),
        P(),
        P(),
        P(),
        P(),
    )
    return jax.shard_map(
        shards,
        mesh=torus,
        in_specs=placed,
        out_specs=(
            P(GX, GY, None, None),
            P(GX_GY, None),
            P(None, GX_GY),
            P(GX_GY, None),
            P(None, GX_GY),
        ),
        check_vma=False,
    )
```

```python
import jax
import jax.numpy as jnp
from jax import lax
from jax.experimental import pallas as pl
from jax.experimental.pallas import tpu as pltpu
from jax.sharding import Mesh
from jax.sharding import PartitionSpec as P

GX_GY = ("gx_0", "gx_1", "gx_2", "gy_0", "gy_1")
GX = ("gx_0", "gx_1", "gx_2")
GY = ("gy_0", "gy_1")

PLACES = ((0, 0), (0, 1), (0, 2), (2, 0), (3, 0), (1, 0), (1, 1), (1, 2))
PARTS = (3, 3, 1, 1)

F = 128
GRP = 512
NGRP = 8
PLANE = 1024
SPAN = 2 * PLANE
EDGES = 3072
HALF = 256
CAP = 128
SENT = 144
ECHUNK = 1024
LOOKED = 256

bf16 = jnp.bfloat16
f32 = jnp.float32


def dot(a, b):
    return jnp.dot(a, b, preferred_element_type=f32)


def dot_nt(a, b):
    return lax.dot_general(a, b, (((1,), (1,)), ((), ())), preferred_element_type=f32)


def silu(v):
    half = 0.5 * v
    return half + half * jnp.tanh(half)


def one_hot(rows, index):
    lanes = index.shape[1]
    mine = lax.broadcasted_iota(jnp.int16, (rows, lanes), 0) == index.astype(jnp.int16)
    return jnp.where(mine, jnp.ones((), bf16), jnp.zeros((), bf16))


def looked_up(table, index):
    lane = jnp.broadcast_to(index & (F - 1), (F, F))
    found = [
        jnp.take_along_axis(table[:, at : at + F], lane, axis=1, mode="promise_in_bounds")
        for at in range(0, GRP, F)
    ]
    odd = (index & F) > 0
    upper = (index & HALF) > 0
    return jnp.where(
        upper, jnp.where(odd, found[3], found[2]), jnp.where(odd, found[1], found[0])
    )


def encode_kernel(state, feat, cell, w_enc, mesh1, y_low, y_high, x_low, x_high):
    g = pl.program_id(0)
    local = cell[0] - g * SPAN
    row = local & (PLANE - 1)
    plane = (local >> 10).astype(f32)
    upper = jnp.transpose(jnp.broadcast_to(plane, (8, GRP)))[:, 0:1]
    rows = dot(feat[...], w_enc[...])
    spread = jnp.concatenate([(rows * (1.0 - upper)).astype(bf16), (rows * upper).astype(bf16)], axis=1)
    added = dot(one_hot(PLANE, row), spread)
    for p in range(2):
        here = pl.ds(p * PLANE, PLANE)
        mesh1[here, :] = (state[here, :].astype(f32) + added[:, p * F : (p + 1) * F]).astype(bf16)
    for p in range(2):
        y_low[p] = mesh1[pl.ds(p * PLANE, 32), :]
        y_high[p] = mesh1[pl.ds(p * PLANE + PLANE - 32, 32), :]

    @pl.when(g == 0)
    def _():
        x_low[...] = mesh1[pl.ds(0, PLANE), :]

    @pl.when(g == NGRP - 1)
    def _():
        x_high[...] = mesh1[pl.ds(PLANE, PLANE), :]


def encode(state, feat, cell3, w_enc):
    full = lambda g: (0, 0)
    part = lambda g: (g, 0)
    return pl.pallas_call(
        encode_kernel,
        grid=(NGRP,),
        in_specs=[
            pl.BlockSpec((SPAN, F), part),
            pl.BlockSpec((GRP, F), part),
            pl.BlockSpec((1, 1, GRP), lambda g: (g, 0, 0)),
            pl.BlockSpec((F, F), full),
        ],
        out_specs=[
            pl.BlockSpec((SPAN, F), part),
            pl.BlockSpec((2, 32, F), lambda g: (g, 0, 0)),
            pl.BlockSpec((2, 32, F), lambda g: (g, 0, 0)),
            pl.BlockSpec((PLANE, F), full),
            pl.BlockSpec((PLANE, F), full),
        ],
        out_shape=[
            jax.ShapeDtypeStruct((NGRP * SPAN, F), bf16),
            jax.ShapeDtypeStruct((2 * NGRP, 32, F), bf16),
            jax.ShapeDtypeStruct((2 * NGRP, 32, F), bf16),
            jax.ShapeDtypeStruct((PLANE, F), bf16),
            jax.ShapeDtypeStruct((PLANE, F), bf16),
        ],
        compiler_params=pltpu.CompilerParams(dimension_semantics=("arbitrary",)),
        name="encode",
    )(state, feat, cell3, w_enc)


def edge_kernel(feat, pairs, dest, w_pair, w_edge, edge_sum, target, before, taken):
    g = pl.program_id(0)

    @pl.when(g == 0)
    def _():
        i = lax.broadcasted_iota(jnp.int32, (GRP, GRP), 0)
        j = lax.broadcasted_iota(jnp.int32, (GRP, GRP), 1)
        before[...] = jnp.where(i < j, 1.0, 0.0).astype(bf16)
        taken[...] = jnp.zeros((8, F), f32)

    proj = jnp.transpose(dot(feat[...], w_pair[...]).astype(bf16).astype(f32))
    send = proj[:F]
    send_two = jnp.concatenate([proj[:F, :HALF], proj[:F, HALF:]], axis=0).astype(bf16)
    recv = jnp.concatenate([proj[F:, :HALF], proj[F:, HALF:]], axis=0).astype(bf16)
    total = jnp.zeros((HALF, 2 * F), f32)
    for at in range(0, EDGES, ECHUNK):
        s = pairs[0:1, pl.ds(at, ECHUNK)]
        r = pairs[1:2, pl.ds(at, ECHUNK)]
        hot_r = one_hot(HALF, r & (HALF - 1))
        up_r = (r & HALF) > 0
        zero = jnp.zeros((), bf16)
        rest = s[:, LOOKED:]
        by_product = dot(send_two, one_hot(HALF, rest & (HALF - 1)))
        from_s = jnp.concatenate(
            [looked_up(send, s[:, i : i + F]) for i in range(0, LOOKED, F)]
            + [jnp.where((rest & HALF) > 0, by_product[F:], by_product[:F])],
            axis=1,
        )
        from_r = dot(recv, hot_r)
        act = silu(
            from_s + jnp.where(up_r, from_r[F:], from_r[:F])
        )
        act = act.astype(bf16)
        spread = jnp.concatenate([jnp.where(up_r, zero, act), jnp.where(up_r, act, zero)], axis=0)
        total = total + dot(hot_r, jnp.transpose(spread))
    summed = jnp.concatenate([total[:, :F], total[:, F:]], axis=0)
    high = summed.astype(bf16)
    low = (summed - high.astype(f32)).astype(bf16)
    edge_sum[...] = (dot(high, w_edge[...]) + dot(low, w_edge[...])).astype(bf16)

    way = dest[0]
    ways = lax.broadcasted_iota(jnp.int32, (8, GRP), 0)
    mine = jnp.where(ways + 1 == way, 1.0, 0.0)
    earlier = dot(mine.astype(bf16), before[...]) + taken[:, 0:1]
    slot = jnp.sum(mine * (earlier + (ways * CAP).astype(f32)), axis=0, keepdims=True)
    target[0] = jnp.where(way > 0, slot, -1.0).astype(jnp.int32)
    taken[...] = taken[...] + jnp.sum(mine, axis=1, keepdims=True)


def edges(feat, pairs, dest3, w_pair, w_edge):
    full = lambda g: (0, 0)
    part = lambda g: (g, 0)
    row = lambda g: (g, 0, 0)
    return pl.pallas_call(
        edge_kernel,
        grid=(NGRP,),
        in_specs=[
            pl.BlockSpec((GRP, F), part),
            pl.BlockSpec((2, EDGES), lambda g: (0, g)),
            pl.BlockSpec((1, 1, GRP), row),
            pl.BlockSpec((F, 2 * F), full),
            pl.BlockSpec((F, F), full),
        ],
        out_specs=[pl.BlockSpec((GRP, F), part), pl.BlockSpec((1, 1, GRP), row)],
        out_shape=[
            jax.ShapeDtypeStruct((NGRP * GRP, F), bf16),
            jax.ShapeDtypeStruct((NGRP, 1, GRP), jnp.int32),
        ],
        scratch_shapes=[pltpu.VMEM((GRP, GRP), bf16), pltpu.VMEM((8, F), f32)],
        compiler_params=pltpu.CompilerParams(dimension_semantics=("arbitrary",)),
        name="edges",
    )(feat, pairs, dest3, w_pair, w_edge)


def node_kernel(
    before,
    here,
    after,
    x_low,
    x_high,
    y_low,
    y_high,
    feat,
    edge_sum,
    cell,
    dest,
    target,
    mass,
    velocity,
    w_mesh,
    w_node,
    w_accel,
    mesh_out,
    stay_feat,
    vel1_out,
    totals,
    *rest,
):
    packed = rest[:4]
    moved, riding, sums = rest[4:]
    g = pl.program_id(0)
    first = g == 0
    final = g == NGRP - 1

    @pl.when(first)
    def _():
        moved[...] = jnp.zeros_like(moved)
        riding[...] = jnp.zeros_like(riding)
        sums[...] = jnp.zeros_like(sums)

    chunk = 256
    z = lax.broadcasted_iota(jnp.int32, (chunk, F), 0) & 31
    for p in range(2):
        base = p * PLANE
        for at in range(0, PLANE, chunk):
            rows = pl.ds(at, chunk)
            mine = here[pl.ds(base + at, chunk), :].astype(f32)
            if p == 0:
                below = jnp.where(first, x_low[rows, :], before[rows, :])
                above = here[pl.ds(PLANE + at, chunk), :]
            else:
                below = here[rows, :]
                above = jnp.where(final, x_high[rows, :], after[rows, :])
            if at == 0:
                left = jnp.concatenate([y_low[p], here[pl.ds(base, chunk - 32), :]], axis=0)
            else:
                left = here[pl.ds(base + at - 32, chunk), :]
            if at + chunk == PLANE:
                right = jnp.concatenate([here[pl.ds(base + at + 32, chunk - 32), :], y_high[p]], axis=0)
            else:
                right = here[pl.ds(base + at + 32, chunk), :]
            down = jnp.where(z == 0, 0.0, pltpu.roll(mine, 1, 0))
            up = jnp.where(z == 31, 0.0, pltpu.roll(mine, chunk - 1, 0))
            sides = (
                (below.astype(f32) + above.astype(f32))
                + (left.astype(f32) + right.astype(f32))
                + (down + up)
            ).astype(bf16)
            mesh_out[pl.ds(base + at, chunk), :] = (mine + silu(dot(sides, w_mesh[...]))).astype(bf16)

    local = cell[0] - g * SPAN
    way = dest[0]
    ways = lax.broadcasted_iota(jnp.int32, (8, GRP), 0)
    row = (local & (PLANE - 1)).astype(f32)
    plane = (local >> 10).astype(f32)
    stays = jnp.where(way == 0, 1.0, 0.0)
    three = jnp.where(ways == 0, row, jnp.where(ways == 1, plane, jnp.where(ways == 2, stays, way.astype(f32))))
    columns = jnp.transpose(three)
    row_at = columns[:, 0:1].astype(jnp.int32)
    upper = columns[:, 1:2]
    stay = columns[:, 2:3]
    both = jnp.concatenate([mesh_out[pl.ds(0, PLANE), :], mesh_out[pl.ds(PLANE, PLANE), :]], axis=1)
    column = jnp.broadcast_to(row_at, (GRP, F)).astype(jnp.int16)
    lane = lax.broadcasted_iota(jnp.int16, (GRP, F), 1)
    one, zero = jnp.ones((), bf16), jnp.zeros((), bf16)
    hot = jnp.concatenate(
        [jnp.where(lane + jnp.int16(at) == column, one, zero) for at in range(0, PLANE, F)], axis=1
    )
    found = dot(hot, both)
    near = jnp.where(upper > 0.5, found[:, F:], found[:, :F]).astype(bf16)
    update = dot(edge_sum[...], w_node[:F, :]) + dot(near, w_node[F:, :])
    h = (feat[...].astype(f32) + silu(update)).astype(bf16)
    stay_feat[...] = jnp.where(stay > 0.5, h.astype(f32), 0.0).astype(bf16)
    vel1 = velocity[...] + dot_nt(w_accel[...], h)
    vel1_out[...] = vel1
    weight = mass[0]
    sums[0:3, :] = sums[0:3, :] + weight * vel1
    sums[3:4, :] = sums[3:4, :] + weight

    extra = jnp.concatenate([vel1, weight, jnp.zeros((12, GRP), f32)], axis=0)
    extras = jnp.concatenate([jnp.where(way == k + 1, extra, 0.0) for k in range(8)], axis=0)
    extras = jnp.transpose(extras).astype(bf16)
    goes = columns[:, 3:4]
    full = h.astype(f32)
    halves = jnp.concatenate(
        [
            jnp.where((goes > 0.5) & (goes < 4.5), full, 0.0).astype(bf16),
            jnp.where(goes > 4.5, full, 0.0).astype(bf16),
        ],
        axis=1,
    )
    to = target[0]
    moved[...] = moved[...] + dot(one_hot(4 * CAP, to & (4 * CAP - 1)), halves)
    riding[...] = riding[...] + dot(one_hot(CAP, to & (CAP - 1)), extras)

    @pl.when(final)
    def _():
        column = jnp.broadcast_to(jnp.sum(sums[...], axis=1, keepdims=True), (8, F))
        totals[...] = jnp.broadcast_to(jnp.transpose(column)[0:1, 0:4], (F, 4))[:, None, :]
        rode = jnp.transpose(riding[...]).astype(bf16)
        for k in range(8):
            rows = pl.ds(k % 4 * CAP, CAP)
            lanes = pl.ds(k // 4 * F, F)
            to, place = PLACES[k]
            packed[to][pl.ds(place * SENT, CAP), :] = moved[rows, lanes].astype(bf16)
            packed[to][pl.ds(place * SENT + CAP, SENT - CAP), :] = rode[k * 16 : (k + 1) * 16]


def nodes(mesh1, halos, feat, edge_sum, cell3, dest3, target, mass3, velocity, w_mesh, w_node, w_accel):
    full = lambda g: (0, 0)
    part = lambda g: (g, 0)
    row = lambda g: (g, 0, 0)
    x_low, x_high, y_low, y_high = halos
    return pl.pallas_call(
        node_kernel,
        grid=(NGRP,),
        in_specs=[
            pl.BlockSpec((PLANE, F), lambda g: (jnp.maximum(2 * g - 1, 0), 0)),
            pl.BlockSpec((SPAN, F), part),
            pl.BlockSpec((PLANE, F), lambda g: (jnp.minimum(2 * g + 2, 2 * NGRP - 1), 0)),
            pl.BlockSpec((PLANE, F), full),
            pl.BlockSpec((PLANE, F), full),
            pl.BlockSpec((2, 32, F), row),
            pl.BlockSpec((2, 32, F), row),
            pl.BlockSpec((GRP, F), part),
            pl.BlockSpec((GRP, F), part),
            pl.BlockSpec((1, 1, GRP), row),
            pl.BlockSpec((1, 1, GRP), row),
            pl.BlockSpec((1, 1, GRP), row),
            pl.BlockSpec((1, 1, GRP), row),
            pl.BlockSpec((3, GRP), lambda g: (0, g)),
            pl.BlockSpec((F, F), full),
            pl.BlockSpec((2 * F, F), full),
            pl.BlockSpec((3, F), full),
        ],
        out_specs=[
            pl.BlockSpec((SPAN, F), part),
            pl.BlockSpec((GRP, F), part),
            pl.BlockSpec((3, GRP), lambda g: (0, g)),
            pl.BlockSpec((F, 1, 4), lambda g: (0, 0, 0)),
        ]
        + [pl.BlockSpec((n * SENT, F), full) for n in PARTS],
        out_shape=[
            jax.ShapeDtypeStruct((NGRP * SPAN, F), bf16),
            jax.ShapeDtypeStruct((NGRP * GRP, F), bf16),
            jax.ShapeDtypeStruct((3, NGRP * GRP), f32),
            jax.ShapeDtypeStruct((F, 1, 4), f32),
        ]
        + [jax.ShapeDtypeStruct((n * SENT, F), bf16) for n in PARTS],
        scratch_shapes=[pltpu.VMEM((4 * CAP, 2 * F), f32), pltpu.VMEM((CAP, F), f32), pltpu.VMEM((8, GRP), f32)],
        compiler_params=pltpu.CompilerParams(dimension_semantics=("arbitrary",)),
        name="nodes",
    )(
        mesh1,
        mesh1,
        mesh1,
        x_low,
        x_high,
        y_low,
        y_high,
        feat,
        edge_sum,
        cell3,
        dest3,
        target,
        mass3,
        velocity,
        w_mesh,
        w_node,
        w_accel,
    )


def near(block):
    return pltpu.with_memory_space_constraint(block, pltpu.VMEM)


def relay_kernel(from_high, from_low, own_down, own_up, down, up):
    for ref, own, at in ((down, own_down, 0), (up, own_up, 2)):
        there = pl.ds(at * SENT, SENT)
        ref[0:SENT, :] = from_high[there, :]
        ref[SENT : 2 * SENT, :] = own[...]
        ref[2 * SENT : 3 * SENT, :] = from_low[there, :]


def relay(from_high, from_low, own_down, own_up):
    return pl.pallas_call(
        relay_kernel,
        out_shape=[jax.ShapeDtypeStruct((3 * SENT, F), bf16)] * 2,
        name="relay",
    )(from_high, from_low, own_down, own_up)


def finish_kernel(from_high, from_low, down, up, totals, vel1, dest, arrived_feat, arrived_vel, stay_vel):
    total = jnp.transpose(jnp.broadcast_to(jnp.sum(totals[...], axis=0), (8, 4)))
    drift = total[0:3, 0:1] / total[3:4, 0:1]
    stay_vel[...] = jnp.where(dest[...] == 0, vel1[...] - drift, 0.0)
    sources = (
        (down, 0),
        (from_high, 1),
        (up, 0),
        (down, 1),
        (up, 1),
        (down, 2),
        (from_low, 1),
        (up, 2),
    )
    for k, (ref, at) in enumerate(sources):
        arrived_feat[pl.ds(k * CAP, CAP), :] = ref[pl.ds(at * SENT, CAP), :]
        extra = ref[pl.ds(at * SENT + CAP, SENT - CAP), :].astype(f32)
        weight = extra[3:4]
        arrived_vel[0:3, pl.ds(k * CAP, CAP)] = jnp.where(weight > 0, extra[0:3] - drift, 0.0)
        arrived_vel[3:4, pl.ds(k * CAP, CAP)] = weight


def finish(*args):
    return pl.pallas_call(
        finish_kernel,
        out_shape=[
            jax.ShapeDtypeStruct((8 * CAP, F), bf16),
            jax.ShapeDtypeStruct((4, 8 * CAP), f32),
            jax.ShapeDtypeStruct((3, NGRP * GRP), f32),
        ],
        name="finish",
    )(*args)


def ring(block, axis, step):
    size = lax.axis_size(axis)
    return lax.ppermute(block, axis, [(i, (i + step) % size) for i in range(size)])


def shards(
    mesh_state,
    part_feat,
    cell_index,
    pairs,
    dest,
    mass,
    velocity,
    w_enc,
    w_mesh,
    w_pair,
    w_edge,
    w_node,
    w_accel,
):
    shape = mesh_state.shape
    cell3 = cell_index.reshape(NGRP, 1, GRP)
    dest3 = dest.reshape(NGRP, 1, GRP)
    mass3 = mass.reshape(NGRP, 1, GRP)
    mesh1, y_first, y_last, x_first, x_last = encode(
        mesh_state.reshape(-1, F), part_feat, cell3, w_enc
    )
    halos = (ring(x_last, GX, 1), ring(x_first, GX, -1), ring(y_last, GY, 1), ring(y_first, GY, -1))
    halos = tuple(near(block) for block in halos)
    edge_sum, target = edges(part_feat, pairs, dest3, w_pair, w_edge)
    mesh_out, stay_feat, vel1, totals, *packed = nodes(
        mesh1, halos, part_feat, edge_sum, cell3, dest3, target, mass3, velocity, w_mesh, w_node, w_accel
    )
    to_low, to_high, own_down, own_up = packed
    from_high, from_low = ring(to_low, GX, -1), ring(to_high, GX, 1)
    from_high, from_low = near(from_high), near(from_low)
    down, up = relay(from_high, from_low, own_down, own_up)
    down, up, totals = lax.optimization_barrier((down, up, totals))
    down, up = ring(down, GY, -1), ring(up, GY, 1)
    totals = lax.all_to_all(totals, GX_GY, 0, 0)
    down, up = near(down), near(up)
    arrived_feat, arrived_vel, stay_vel = finish(
        from_high, from_low, down, up, totals, vel1, dest.reshape(1, -1)
    )
    return (mesh_out.reshape(shape), stay_feat, stay_vel, arrived_feat, arrived_vel)


def solution(mesh):
    torus = Mesh(mesh.devices.reshape(2, 4, 2, 4, 2), ("gx_0", "gx_1", "gx_2", "gy_0", "gy_1"))
    placed = (
        P(GX, GY, None, None),
        P(GX_GY, None),
        P(GX_GY),
        P(None, GX_GY),
        P(GX_GY),
        P(GX_GY),
        P(None, GX_GY),
        P(),
        P(),
        P(),
        P(),
        P(),
        P(),
    )
    return jax.shard_map(
        shards,
        mesh=torus,
        in_specs=placed,
        out_specs=(
            P(GX, GY, None, None),
            P(GX_GY, None),
            P(None, GX_GY),
            P(GX_GY, None),
            P(None, GX_GY),
        ),
        check_vma=False,
    )
```
